512 devices in a mesh: parts: 2 (over y), space: 16 (over z), tm: 8 (over x), chan: 2 (over core).
Axes of the slice: x: 8, y: 2, z: 16, core: 2. Of those that a mesh axis runs over, the one named last changes fastest.
The devices are a block of a 8x16x16 slice.
Arguments:
- events: int32 [64, 128, 128], P(('parts', 'tm'), 'space'), parts along dimension 0, may hold values 0 or 1
- soft_info: bfloat16 [64, 128, 128], P(('parts', 'tm'), 'space'), parts along dimension 0, may hold values from -6 to 6
- embed: float32 [4, 64], replicated, may hold values from -6 to 6
- soft_gain: float32 [64], replicated, may hold values from -6 to 6
- conv_weights: bfloat16 [3, 64, 1728], replicated, may hold values from -0.21875 to 0.21875
- conv_bias: float32 [3, 64], replicated, may hold values from -1.75 to 1.75
- readout_weight: float32 [64], replicated, may hold values from -0.75 to 0.75
Outputs:
- logits: float32 [64, 128, 128], P(('parts', 'tm'), 'space'), parts along dimension 0
The draws below stay inside these ranges and needn't reach their ends.
There are 2 independent parts, one for each index of `parts`. The reference program is written for one: setup_inputs(seed, part) draws one part's arguments, and reference() takes and returns one part's arrays. A program takes and returns all parts, laid end to end along the dimension named above; an argument that names none is the same for every part. Nothing has to cross between parts.
All inputs are finite; a program needn't handle non-finite values. No bound on the sum of `events` on one device may be relied on, other than what follows from the above.
Results may differ from the reference program's by a relative error of at most 0.024.
Values may be sent and summed in bfloat16 or wider, within the bound.
A program may use at most 64 MiB of HBM per device.

```python
import jax
import jax.numpy as jnp
from jax import lax

CH = 64
GRID = 128
WIN = 2
LAYERS = 3
ROUNDS = 32
N_TM = 8


def place_ends(entries, key, least, top_value):
    shape = entries.shape
    place = [jax.random.randint(jax.random.fold_in(key, axis), (), 0, shape[axis]) for axis in range(len(shape))]
    entries = entries.at[tuple(place)].set(least)
    longest = shape.index(max(shape))
    place[longest] = (place[longest] + 1) % shape[longest]
    return entries.at[tuple(place)].set(top_value)


def block_scale(key, extent, pieces, least, top_value):
    def one(dim, parts):
        heights = jax.random.uniform(jax.random.fold_in(jax.random.fold_in(key, 6), dim), (parts,), jnp.float32, least / len(pieces), top_value / len(pieces))
        return jnp.repeat(jnp.exp(heights), extent[dim] // parts).reshape((-1,) + (1,) * (len(extent) - dim - 1))

    level = one(*pieces[0])
    for cut in pieces[1:]:
        level = level * one(*cut)
    return level


def normal_values(own_key, dims, deviation, most, split=(), kind=jnp.bfloat16):
    result = jax.random.normal(own_key, dims, jnp.float32) * deviation
    if len(split) > 0:
        result = block_scale(own_key, dims, split, -0.22, 0.18) * result
    return jnp.clip(result, min=-most, max=most).astype(kind)


def setup_inputs(seed: int = 0, part: int = 0) -> dict:
    keys = jax.random.split(jax.random.key(seed), 8)
    own_keys = jax.random.split(jax.random.fold_in(keys[7], part), 8)
    events = place_ends((jax.random.randint(own_keys[0], (ROUNDS, GRID, GRID), 0, 4) < 1).astype(jnp.int32), jax.random.fold_in(own_keys[0], 1), 0, 1)
    soft_info = normal_values(own_keys[1], (ROUNDS, GRID, GRID), 1.0, 6.0, ((0, 8), (1, 16)))
    embed = normal_values(keys[2], (4, CH), 1.0, 6.0, (), jnp.float32)
    soft_gain = normal_values(keys[3], (CH,), 1.0, 6.0, (), jnp.float32)
    conv_weights = normal_values(keys[4], (LAYERS, CH, CH * 27), (CH * 27 // 2) ** -0.5, 0.21875)
    conv_bias = normal_values(keys[5], (LAYERS, CH), 0.3, 1.75, (), jnp.float32)
    readout_weight = normal_values(keys[6], (CH,), CH ** -0.5, 0.75, (), jnp.float32)
    return {"events": events, "soft_info": soft_info, "embed": embed, "soft_gain": soft_gain, "conv_weights": conv_weights, "conv_bias": conv_bias, "readout_weight": readout_weight}


def conv_layer(inputs, kernel, bias_row):
    output = lax.conv_general_dilated(inputs, kernel, (1, 1, 1), ((0, 0), (1, 1), (1, 1)), dimension_numbers=("NCDHW", "OIDHW", "NCDHW"), preferred_element_type=jnp.float32)
    return jnp.maximum(output + bias_row[None, :, None, None, None], 0.0).astype(jnp.bfloat16)


def run_window(hidden, front, back, kernels, conv_bias):
    for layer in range(LAYERS):
        hidden = conv_layer(jnp.concatenate([front, hidden, back], 2), kernels[layer], conv_bias[layer])
    return hidden


def reference(events, soft_info, embed, soft_gain, conv_weights, conv_bias, readout_weight):
    positions = jnp.arange(GRID, dtype=jnp.int32)
    parity = (positions[:, None] + positions[None, :]) % 2
    code = 2 * parity[None] + events
    onehot = (code[None] == jnp.arange(4, dtype=jnp.int32)[:, None, None, None]).astype(jnp.float32)
    start = jnp.einsum('kc,kryx->cryx', embed, onehot) + soft_gain[:, None, None, None] * soft_info.astype(jnp.float32)[None]
    start = start.astype(jnp.bfloat16)
    windows = start.reshape(CH, N_TM, 2, WIN, GRID, GRID)
    first = jnp.transpose(windows[:, :, 0], (1, 0, 2, 3, 4))
    second = jnp.transpose(windows[:, :, 1], (1, 0, 2, 3, 4))
    kernels = conv_weights.reshape(LAYERS, CH, CH, 3, 3, 3)
    zeros = jnp.zeros((N_TM, CH, 1, GRID, GRID), jnp.bfloat16)
    first = run_window(first, zeros, zeros, kernels, conv_bias)
    after = jnp.concatenate([first[1:, :, :1], zeros[:1]], 0)
    second = run_window(second, first[:, :, -1:], after, kernels, conv_bias)
    stacked = jnp.stack([first, second], 1)
    logits = jnp.einsum('c,nscwyx->nswyx', readout_weight, stacked.astype(jnp.float32))
    return logits.reshape(ROUNDS, GRID, GRID)
```

```python
import functools

import jax
import jax.numpy as jnp
from jax import lax
from jax.experimental import pallas as pl
from jax.experimental.pallas import tpu as pltpu
from jax.sharding import PartitionSpec as P

F32 = jnp.float32
BF16 = jnp.bfloat16
MESH = pl.DeviceIdType.MESH


def iota(shape, dim):
    return lax.broadcasted_iota(jnp.int32, shape, dim)


def three_terms(value):
    high = value.astype(BF16)
    rest = value - high.astype(F32)
    middle = rest.astype(BF16)
    low = (rest - middle.astype(F32)).astype(BF16)
    return high, middle, low


def one_hot(condition):
    return jnp.where(condition, 1.0, 0.0).astype(BF16)


def dot(a, b):
    return lax.dot_general(a, b, (((1,), (0,)), ((), ())), preferred_element_type=F32)


def dot_nt(a, b):
    return lax.dot_general(a, b, (((1,), (1,)), ((), ())), preferred_element_type=F32)


def dot_tn(a, b):
    return lax.dot_general(a, b, (((0,), (0,)), ((), ())), preferred_element_type=F32)


def quad(row):
    return jnp.concatenate([row] * 4, axis=1)


def put(ref, lead, value, count):
    width = value.shape[2]
    q = iota((count, 16, width), 1)
    last, first = value[:, 112:128], value[:, 0:16]
    before = jnp.where(q == 0, 0.0, pltpu.roll(last, 1, 1))
    after = jnp.where(q == 15, 0.0, pltpu.roll(first, 15, 1))
    ref[(*lead, pl.ds(0, count), pl.ds(0, 16))] = before.astype(BF16)
    ref[(*lead, pl.ds(0, count), pl.ds(16, 128))] = value.astype(BF16)
    ref[(*lead, pl.ds(0, count), pl.ds(144, 16))] = after.astype(BF16)


def kernel(
    spaces, times,
    ev_hbm, so_hbm, emb_hbm, gain_hbm, cw_hbm, cb_hbm, rw_hbm,
    out_ref,
    ev, so, emb, gain, cw, cb, rw,
    win, unique, ha, hb, final, paired, mine, theirs,
    load_sem, send_sem, recv_sem,
):
    space, time, core = lax.axis_index("space"), lax.axis_index("tm"), lax.axis_index("chan")
    grid_rows = 8 * spaces
    up, down = space > 0, space < spaces - 1
    later, earlier = time < times - 1, time > 0

    loads = [
        pltpu.make_async_copy(src, dst, load_sem.at[i])
        for i, (src, dst) in enumerate(
            ((ev_hbm, ev), (so_hbm, so), (cw_hbm, cw), (emb_hbm, emb), (gain_hbm, gain), (cb_hbm, cb), (rw_hbm, rw))
        )
    ]
    for load in loads:
        load.start()

    barrier = pltpu.get_barrier_semaphore()

    def greet(there, device):
        @pl.when(there)
        def _():
            pl.semaphore_signal(barrier, inc=1, device_id=device, device_id_type=MESH)

    greet(up, {"space": space - 1})
    greet(down, {"space": space + 1})
    greet(later, {"tm": time + 1})
    greet(earlier, {"tm": time - 1})
    pl.semaphore_signal(barrier, inc=1, device_id={"chan": 1 - core}, device_id_type=MESH)

    spread = one_hot(iota((128, 128), 0) == (iota((128, 128), 1) & 15) * 8 + (iota((128, 128), 1) >> 4))
    m = iota((64, 64), 0)
    source = (
        (m & 1) * 32 + ((m >> 5) * 2 + 1 - ((m >> 2) & 1)) * 8 + ((m >> 3) & 3) * 2 + ((m >> 1) & 1)
    )
    order = one_hot(iota((64, 64), 1) == source)
    loads[0].wait()
    loads[1].wait()
    raw = jnp.concatenate([ev[...].astype(F32).reshape(32, 128), so[...].astype(F32).reshape(32, 128)], axis=0)
    staged = dot(order, dot(raw.astype(BF16), spread).astype(BF16)).reshape(2, 4, 8, 128).astype(BF16)
    win[0, 3:7] = staged[0]
    win[1, 3:7] = staged[1]

    def remote(src, dst, i, device):
        return pltpu.make_async_remote_copy(
            src_ref=src, dst_ref=dst, send_sem=send_sem.at[i], recv_sem=recv_sem.at[i],
            device_id=device, device_id_type=MESH,
        )

    to_below = remote(win.at[0:2, 4:7], win.at[0:2, 0:3], 0, {"space": space + 1})
    to_above = remote(win.at[0:2, 3:6], win.at[0:2, 7:10], 1, {"space": space - 1})
    to_earlier = remote(win.at[0, 3:7], win.at[2, 3:7], 2, {"tm": time - 1})
    on_below = remote(win.at[2, 4:7], win.at[2, 0:3], 3, {"space": space + 1})
    on_above = remote(win.at[2, 3:6], win.at[2, 7:10], 4, {"space": space - 1})
    swap = remote(mine, theirs, 5, {"chan": 1 - core})

    pl.semaphore_wait(
        barrier,
        1 + jnp.where(up, 1, 0) + jnp.where(down, 1, 0) + jnp.where(later, 1, 0) + jnp.where(earlier, 1, 0),
    )
    pl.when(down)(to_below.start)
    pl.when(up)(to_above.start)
    pl.when(earlier)(to_earlier.start)

    loads[2].wait()
    blank = jnp.zeros((3, 1, 3, 16, 128), F32)
    for half in range(4):
        pieces = []
        for chunk in (2 * half, 2 * half + 1):
            begin = 216 * chunk // 128 * 128
            stop = min(-(-(216 * chunk + 216) // 128) * 128, cw.shape[2])
            n = iota((216, stop - begin), 0)
            select = one_hot(iota((216, stop - begin), 1) == (n & 7) * 27 + (n >> 3) + (216 * chunk - begin))
            taps = [cw[layer, :, begin:stop] for layer in range(3)]
            two = dot_nt(select, jnp.concatenate([taps[0], taps[0], taps[1], taps[1]], axis=0))
            one = dot_nt(select, jnp.concatenate([taps[2], taps[2]], axis=0))
            pieces.append([v.reshape(27, 8, 128) for v in (two[:, :128], two[:, 128:], one)])
        for layer in range(3):
            tap = jnp.concatenate([pieces[0][layer], pieces[1][layer]], axis=1).reshape(3, 3, 3, 16, 128)
            low = jnp.concatenate([tap, blank], axis=1)
            high = jnp.concatenate([blank, tap], axis=1)
            both = jnp.where(iota((3, 4, 3, 16, 128), 4) < 64, low, high)
            unique[layer, :, :, :, 16 * half : 16 * half + 16, :] = both.astype(BF16)

    for load in loads[3:]:
        load.wait()
    e_terms = three_terms(quad(emb[...]))
    g_terms = three_terms(quad(gain[...]))
    column = jnp.concatenate(
        [t.astype(F32) for t in e_terms] + [t.astype(F32) for t in g_terms] + [jnp.zeros((1, 256), F32)], axis=0
    )
    make = jnp.where(
        iota((64, 256), 0) >> 4 == iota((64, 256), 1) >> 6, jnp.concatenate([column] * 4, axis=0), 0.0
    ).astype(BF16)
    bias = [quad(cb[layer : layer + 1, :]) for layer in range(3)]

    base = 8 * space + 4 * core
    k = iota((16, 128), 0)
    column_parity = iota((16, 128), 1) >> 4

    def inputs(cell, row, there):
        event, signal = cell
        inside = (row >= 0) & (row < grid_rows) & there
        code = 2 * ((column_parity + row) & 1) + event.astype(jnp.int32)
        value = jnp.where(k < 12, jnp.where(code == (k & 3), 1.0, 0.0), jnp.where(k < 15, signal, 0.0))
        return jnp.where(inside, value, 0.0)

    def start(cells, count, first_row, there):
        columns = []
        for j in range(count):
            blocks = []
            for b in range(4):
                blocks.append(inputs(cells(j, b), first_row + 2 * j + (b & 1), there))
            columns.append(jnp.concatenate(blocks, axis=0).astype(BF16))
        return dot_tn(jnp.concatenate(columns, axis=1), make).reshape(count, 128, 256)

    def taps_of(ref, lead, first, count):
        parts = []
        for shift in range(3):
            for pair in range(2):
                part = ref[(*lead, pl.ds(first + pair, count), pl.ds(16 * shift, 128))]
                parts.append(part.reshape(count * 128, part.shape[-1]))
        return parts

    def within(layer):
        rows = []
        for shift in range(3):
            for pair in range(2):
                for r in (1, 0):
                    for y in range(2):
                        rows.append(
                            jnp.concatenate(
                                [unique[layer, r + 1 - to, 2 * pair + y, shift] for to in (1, 0)], axis=1
                            )
                        )
        return jnp.concatenate(rows, axis=0)

    def across(layer):
        rows = []
        none = jnp.zeros((64, 128), BF16)
        for shift in range(3):
            for pair in range(2):
                for y in range(2):
                    rows.append(jnp.concatenate([none, unique[layer, 0, 2 * pair + y, shift]], axis=1))
                for y in range(2):
                    rows.append(jnp.concatenate([unique[layer, 2, 2 * pair + y, shift], none], axis=1))
        return jnp.concatenate(rows, axis=0)

    def finish(total, layer, count, first_row, there):
        row = first_row + 2 * iota((count, 1, 256), 0) + ((iota((count, 1, 256), 2) >> 6) & 1)
        inside = (row >= 0) & (row < grid_rows) & there
        value = jnp.maximum(total + bias[layer], 0.0).reshape(count, 128, 256)
        return value * jnp.where(inside, 1.0, 0.0)

    pl.when(later)(to_earlier.wait_recv)
    pl.when(later & down)(on_below.start)
    pl.when(later & up)(on_above.start)
    pl.when(up)(to_below.wait_recv)
    pl.when(down)(to_above.wait_recv)

    def first_kind(w, carry):
        there = (w == 0) | later

        @pl.when((w == 1) & later & up)
        def _():
            on_below.wait_recv()

        @pl.when((w == 1) & later & down)
        def _():
            on_above.wait_recv()

        def cells(j, b):
            tile = win[2 * w, 2 * core + j].astype(F32)
            return tile[2 * b : 2 * b + 1], tile[2 * b + 1 : 2 * b + 2]

        put(ha, (), start(cells, 8, base - 6, there), 8)
        total = dot(jnp.concatenate(taps_of(ha, (), 0, 7), axis=1), within(0))
        put(hb, (), finish(total, 0, 7, base - 5, there), 7)
        total = dot(jnp.concatenate(taps_of(hb, (), 0, 6), axis=1), within(1))
        put(ha, (), finish(total, 1, 6, base - 4, there), 6)
        total = dot(jnp.concatenate(taps_of(ha, (), 0, 5), axis=1), within(2))
        value = finish(total, 2, 5, base - 3, there)
        put(final, (w,), value, 5)
        swapped = jnp.where((iota((4, 128, 256), 2) & 64) == 0, value[1:5], value[0:4])
        put(
            paired, (w,),
            jnp.concatenate([pltpu.roll(swapped[:, :, :128], 64, 2), pltpu.roll(swapped[:, :, 128:], 64, 2)], axis=2),
            4,
        )
        return carry

    lax.fori_loop(0, 2, first_kind, 0)

    def beside(ref, first, count):
        left = taps_of(ref.at[0, :, :, 0:128], (), first, count)
        right = taps_of(ref.at[1, :, :, 128:256], (), first, count)
        return [v for pair in zip(left, right) for v in pair]

    def second(own, others, layer, count, first_other):
        lhs = jnp.concatenate(taps_of(own, (), 0, count) + beside(others, first_other, count), axis=1)
        return dot(lhs, jnp.concatenate([within(layer), across(layer)], axis=0))

    def late_cells(j, b):
        tile = win[1, 2 * core + 1 + j + (b & 1)].astype(F32)
        at = (b >> 1) * 4 + (1 - (b & 1)) * 2
        return tile[at : at + 1], tile[at + 1 : at + 2]

    put(ha, (), start(late_cells, 5, base - 3, True), 5)
    put(hb, (), finish(second(ha, final, 0, 4, 0), 0, 4, base - 2, True), 4)
    put(ha, (), finish(second(hb, paired, 1, 3, 0), 1, 3, base - 1, True), 3)
    last = finish(second(ha, final, 2, 2, 1), 2, 2, base, True).astype(BF16).reshape(256, 256)

    w_terms = three_terms(quad(rw[...]))
    n = iota((32, 256), 0)
    weight = jnp.where(n >> 3 == 0, w_terms[0].astype(F32), jnp.where(n >> 3 == 1, w_terms[1].astype(F32), w_terms[2].astype(F32)))
    weight = jnp.where((n < 24) & ((n & 7) == iota((32, 256), 1) >> 6), weight, 0.0).astype(BF16)
    a_sum = dot_nt(weight, final[0, 1:4, 16:144, :].reshape(384, 256))
    b_sum = dot_nt(weight, last)
    a_sum = a_sum[0:8] + a_sum[8:16] + a_sum[16:24]
    b_sum = b_sum[0:8] + b_sum[8:16] + b_sum[16:24]
    y = iota((8, 128), 0) & 3
    rounds = []
    for total, shift in ((a_sum, 1), (b_sum, 0)):
        for r in range(2):
            rows = []
            for i in range(4):
                pair, inner = (i + shift) // 2, (i + shift) % 2
                b = (1 - r) * 2 + inner
                rows.append(jnp.broadcast_to(total[b : b + 1, 128 * pair : 128 * pair + 128], (8, 128)))
            rounds.append(jnp.where(y < 2, jnp.where(y == 0, rows[0], rows[1]), jnp.where(y == 2, rows[2], rows[3])))
    logits = jnp.concatenate(rounds, axis=0)
    back = one_hot(iota((128, 128), 1) == (iota((128, 128), 0) & 15) * 8 + (iota((128, 128), 0) >> 4))
    parts = dot(jnp.concatenate(three_terms(logits), axis=0), back)
    logits = (parts[0:32] + parts[32:64] + parts[64:96]).reshape(4, 8, 128)
    mine[...] = logits
    swap.start()
    swap.wait_recv()
    own = (iota((4, 8, 128), 1) >> 2) == core
    out_ref[...] = jnp.where(own, logits, theirs[...])

    pl.when(down)(to_below.wait_send)
    pl.when(up)(to_above.wait_send)
    pl.when(earlier)(to_earlier.wait_send)
    pl.when(later & down)(on_below.wait_send)
    pl.when(later & up)(on_above.wait_send)
    swap.wait_send()


def per_device(spaces, times, events, soft_info, embed, soft_gain, conv_weights, conv_bias, readout_weight):
    layers, channels, taps = conv_weights.shape
    gain = soft_gain.reshape(1, channels)
    readout = readout_weight.reshape(1, channels)
    any_space = pl.BlockSpec(memory_space=pl.ANY)
    return pl.pallas_call(
        functools.partial(kernel, spaces, times),
        out_shape=jax.ShapeDtypeStruct(events.shape, F32),
        in_specs=[any_space] * 7,
        out_specs=pl.BlockSpec(memory_space=pltpu.VMEM),
        scratch_shapes=[
            pltpu.VMEM(events.shape, jnp.int32),
            pltpu.VMEM(soft_info.shape, BF16),
            pltpu.VMEM(embed.shape, F32),
            pltpu.VMEM(gain.shape, F32),
            pltpu.VMEM(conv_weights.shape, BF16),
            pltpu.VMEM(conv_bias.shape, F32),
            pltpu.VMEM(readout.shape, F32),
            pltpu.VMEM((3, 10, 8, 128), BF16),
            pltpu.VMEM((layers, 3, 4, 3, channels, 128), BF16),
            pltpu.VMEM((8, 160, 256), BF16),
            pltpu.VMEM((7, 160, 256), BF16),
            pltpu.VMEM((2, 5, 160, 256), BF16),
            pltpu.VMEM((2, 4, 160, 256), BF16),
            pltpu.VMEM(events.shape, F32),
            pltpu.VMEM(events.shape, F32),
            pltpu.SemaphoreType.DMA((7,)),
            pltpu.SemaphoreType.DMA((6,)),
            pltpu.SemaphoreType.DMA((6,)),
        ],
        compiler_params=pltpu.CompilerParams(collective_id=0, has_side_effects=True, vmem_limit_bytes=48 * 1024 * 1024),
    )(events, soft_info, embed, gain, conv_weights, conv_bias, readout)


def solution(mesh):
    tiled = P(("parts", "tm"), "space", None)
    return jax.shard_map(
        functools.partial(per_device, mesh.shape["space"], mesh.shape["tm"]),
        mesh=mesh, in_specs=(tiled, tiled, P(), P(), P(), P(), P()), out_specs=tiled, check_vma=False,
    )
```

```python
import functools

import jax
import jax.numpy as jnp
from jax import lax
from jax.experimental import pallas as pl
from jax.experimental.pallas import tpu as pltpu
from jax.sharding import PartitionSpec as P

F32 = jnp.float32
BF16 = jnp.bfloat16
MESH = pl.DeviceIdType.MESH
LEAD = 3


def iota(shape, dim):
    return lax.broadcasted_iota(jnp.int32, shape, dim)


def three_terms(value):
    high = value.astype(BF16)
    rest = value - high.astype(F32)
    middle = rest.astype(BF16)
    low = (rest - middle.astype(F32)).astype(BF16)
    return high, middle, low


def one_hot(condition):
    return jnp.where(condition, 1.0, 0.0).astype(BF16)


def dot(a, b):
    return lax.dot_general(a, b, (((1,), (0,)), ((), ())), preferred_element_type=F32)


def dot_nt(a, b):
    return lax.dot_general(a, b, (((1,), (1,)), ((), ())), preferred_element_type=F32)


def dot_tn(a, b):
    return lax.dot_general(a, b, (((0,), (0,)), ((), ())), preferred_element_type=F32)


def quad(row):
    return jnp.concatenate([row] * 4, axis=1)


def put(ref, lead, value, count):
    width = value.shape[2]
    q = iota((count, 16, width), 1)
    last, first = value[:, 112:128], value[:, 0:16]
    before = jnp.where(q == 0, 0.0, pltpu.roll(last, 1, 1))
    after = jnp.where(q == 15, 0.0, pltpu.roll(first, 15, 1))
    ref[(*lead, pl.ds(0, count), pl.ds(0, 16))] = before.astype(BF16)
    ref[(*lead, pl.ds(0, count), pl.ds(16, 128))] = value.astype(BF16)
    ref[(*lead, pl.ds(0, count), pl.ds(144, 16))] = after.astype(BF16)


def compute(
    spaces, space, time, up, down, later, earlier, barrier, grid_rows, remote, loads,
    out_ref, ev, so, emb, gain, cw, cb, rw, win, unique, ha, hb, final, paired, result,
):
    spread = one_hot(iota((128, 128), 0) == (iota((128, 128), 1) & 15) * 8 + (iota((128, 128), 1) >> 4))
    m = iota((64, 64), 0)
    source = (
        (m & 1) * 32 + ((m >> 5) * 2 + 1 - ((m >> 2) & 1)) * 8 + ((m >> 3) & 3) * 2 + ((m >> 1) & 1)
    )
    order = one_hot(iota((64, 64), 1) == source)
    loads[0].wait()
    loads[1].wait()
    raw = jnp.concatenate([ev[...].astype(F32).reshape(32, 128), so[...].astype(F32).reshape(32, 128)], axis=0)
    staged = dot(order, dot(raw.astype(BF16), spread).astype(BF16)).reshape(2, 4, 8, 128).astype(BF16)
    win[0, 3:7] = staged[0]
    win[1, 3:7] = staged[1]

    to_below = remote(win.at[0:2, 4:7], win.at[0:2, 0:3], 0, 0, {"space": space + 1})
    to_above = remote(win.at[0:2, 3:6], win.at[0:2, 7:10], 1, 1, {"space": space - 1})
    to_earlier = remote(win.at[0, 3:7], win.at[2, 3:7], 2, 2, {"tm": time - 1})
    on_below = remote(win.at[2, 4:7], win.at[2, 0:3], 3, 3, {"space": space + 1})
    on_above = remote(win.at[2, 3:6], win.at[2, 7:10], 4, 4, {"space": space - 1})

    pl.semaphore_wait(
        barrier,
        jnp.where(up, 1, 0) + jnp.where(down, 1, 0) + jnp.where(later, 1, 0) + jnp.where(earlier, 1, 0),
    )
    pl.when(down)(to_below.start)
    pl.when(up)(to_above.start)
    pl.when(earlier)(to_earlier.start)

    loads[2].wait()
    blank = jnp.zeros((3, 1, 3, 16, 128), F32)
    for half in range(4):
        pieces = []
        for chunk in (2 * half, 2 * half + 1):
            begin = 216 * chunk // 128 * 128
            stop = min(-(-(216 * chunk + 216) // 128) * 128, cw.shape[2])
            n = iota((216, stop - begin), 0)
            select = one_hot(iota((216, stop - begin), 1) == (n & 7) * 27 + (n >> 3) + (216 * chunk - begin))
            taps = [cw[layer, :, begin:stop] for layer in range(3)]
            two = dot_nt(select, jnp.concatenate([taps[0], taps[0], taps[1], taps[1]], axis=0))
            one = dot_nt(select, jnp.concatenate([taps[2], taps[2]], axis=0))
            pieces.append([v.reshape(27, 8, 128) for v in (two[:, :128], two[:, 128:], one)])
        for layer in range(3):
            tap = jnp.concatenate([pieces[0][layer], pieces[1][layer]], axis=1).reshape(3, 3, 3, 16, 128)
            low = jnp.concatenate([tap, blank], axis=1)
            high = jnp.concatenate([blank, tap], axis=1)
            both = jnp.where(iota((3, 4, 3, 16, 128), 4) < 64, low, high)
            unique[layer, :, :, :, 16 * half : 16 * half + 16, :] = both.astype(BF16)

    for load in loads[3:]:
        load.wait()
    e_terms = three_terms(quad(emb[...]))
    g_terms = three_terms(quad(gain[...]))
    column = jnp.concatenate(
        [t.astype(F32) for t in e_terms] + [t.astype(F32) for t in g_terms] + [jnp.zeros((1, 256), F32)], axis=0
    )
    make = jnp.where(
        iota((64, 256), 0) >> 4 == iota((64, 256), 1) >> 6, jnp.concatenate([column] * 4, axis=0), 0.0
    ).astype(BF16)
    bias = [quad(cb[layer : layer + 1, :]) for layer in range(3)]

    base = 8 * space
    k = iota((16, 128), 0)
    column_parity = iota((16, 128), 1) >> 4

    def inputs(cell, row, there):
        event, signal = cell
        inside = (row >= 0) & (row < grid_rows) & there
        code = 2 * ((column_parity + row) & 1) + event.astype(jnp.int32)
        value = jnp.where(k < 12, jnp.where(code == (k & 3), 1.0, 0.0), jnp.where(k < 15, signal, 0.0))
        return jnp.where(inside, value, 0.0)

    def start(cells, count, first_row, there):
        columns = []
        for j in range(count):
            blocks = []
            for b in range(4):
                blocks.append(inputs(cells(j, b), first_row + 2 * j + (b & 1), there))
            columns.append(jnp.concatenate(blocks, axis=0).astype(BF16))
        return dot_tn(jnp.concatenate(columns, axis=1), make).reshape(count, 128, 256)

    def taps_of(ref, lead, first, count):
        parts = []
        for shift in range(3):
            for pair in range(2):
                part = ref[(*lead, pl.ds(first + pair, count), pl.ds(16 * shift, 128))]
                parts.append(part.reshape(count * 128, part.shape[-1]))
        return parts

    def within(layer):
        rows = []
        for shift in range(3):
            for pair in range(2):
                for r in (1, 0):
                    for y in range(2):
                        rows.append(
                            jnp.concatenate(
                                [unique[layer, r + 1 - to, 2 * pair + y, shift] for to in (1, 0)], axis=1
                            )
                        )
        return jnp.concatenate(rows, axis=0)

    def across(layer):
        rows = []
        none = jnp.zeros((64, 128), BF16)
        for shift in range(3):
            for pair in range(2):
                for y in range(2):
                    rows.append(jnp.concatenate([none, unique[layer, 0, 2 * pair + y, shift]], axis=1))
                for y in range(2):
                    rows.append(jnp.concatenate([unique[layer, 2, 2 * pair + y, shift], none], axis=1))
        return jnp.concatenate(rows, axis=0)

    def finish(total, layer, count, first_row, there):
        row = first_row + 2 * iota((count, 1, 256), 0) + ((iota((count, 1, 256), 2) >> 6) & 1)
        inside = (row >= 0) & (row < grid_rows) & there
        value = jnp.maximum(total + bias[layer], 0.0).reshape(count, 128, 256)
        return value * jnp.where(inside, 1.0, 0.0)

    pl.when(later)(to_earlier.wait_recv)
    pl.when(later & down)(on_below.start)
    pl.when(later & up)(on_above.start)
    pl.when(up)(to_below.wait_recv)
    pl.when(down)(to_above.wait_recv)

    def first_kind(w, carry):
        there = (w == 0) | later

        @pl.when((w == 1) & later & up)
        def _():
            on_below.wait_recv()

        @pl.when((w == 1) & later & down)
        def _():
            on_above.wait_recv()

        def cells(j, b):
            tile = win[2 * w, j].astype(F32)
            return tile[2 * b : 2 * b + 1], tile[2 * b + 1 : 2 * b + 2]

        put(ha, (), start(cells, 10, base - 6, there), 10)
        total = dot(jnp.concatenate(taps_of(ha, (), 0, 9), axis=1), within(0))
        put(hb, (), finish(total, 0, 9, base - 5, there), 9)
        total = dot(jnp.concatenate(taps_of(hb, (), 0, 8), axis=1), within(1))
        put(ha, (), finish(total, 1, 8, base - 4, there), 8)
        total = dot(jnp.concatenate(taps_of(ha, (), 0, 7), axis=1), within(2))
        value = finish(total, 2, 7, base - 3, there)
        put(final, (w,), value, 7)
        swapped = jnp.where((iota((6, 128, 256), 2) & 64) == 0, value[1:7], value[0:6])
        put(
            paired, (w,),
            jnp.concatenate([pltpu.roll(swapped[:, :, :128], 64, 2), pltpu.roll(swapped[:, :, 128:], 64, 2)], axis=2),
            6,
        )
        return carry

    lax.fori_loop(0, 2, first_kind, 0)

    def beside(ref, first, count):
        left = taps_of(ref.at[0, :, :, 0:128], (), first, count)
        right = taps_of(ref.at[1, :, :, 128:256], (), first, count)
        return [v for pair in zip(left, right) for v in pair]

    def second(own, others, layer, count, first_other):
        lhs = jnp.concatenate(taps_of(own, (), 0, count) + beside(others, first_other, count), axis=1)
        return dot(lhs, jnp.concatenate([within(layer), across(layer)], axis=0))

    def late_cells(j, b):
        tile = win[1, 1 + j + (b & 1)].astype(F32)
        at = (b >> 1) * 4 + (1 - (b & 1)) * 2
        return tile[at : at + 1], tile[at + 1 : at + 2]

    put(ha, (), start(late_cells, 7, base - 3, True), 7)
    put(hb, (), finish(second(ha, final, 0, 6, 0), 0, 6, base - 2, True), 6)
    put(ha, (), finish(second(hb, paired, 1, 5, 0), 1, 5, base - 1, True), 5)
    last = finish(second(ha, final, 2, 4, 1), 2, 4, base, True).astype(BF16).reshape(512, 256)

    w_terms = three_terms(quad(rw[...]))
    n = iota((32, 256), 0)
    weight = jnp.where(n >> 3 == 0, w_terms[0].astype(F32), jnp.where(n >> 3 == 1, w_terms[1].astype(F32), w_terms[2].astype(F32)))
    weight = jnp.where((n < 24) & ((n & 7) == iota((32, 256), 1) >> 6), weight, 0.0).astype(BF16)
    a_sum = dot_nt(weight, final[0, 1:6, 16:144, :].reshape(640, 256))
    b_sum = dot_nt(weight, last)
    a_sum = a_sum[0:8] + a_sum[8:16] + a_sum[16:24]
    b_sum = b_sum[0:8] + b_sum[8:16] + b_sum[16:24]
    y = iota((8, 128), 0)
    rounds = []
    for total, shift in ((a_sum, 1), (b_sum, 0)):
        for r in range(2):
            tile = jnp.zeros((8, 128), F32)
            for i in range(8):
                pair, inner = (i + shift) // 2, (i + shift) % 2
                b = (1 - r) * 2 + inner
                row = jnp.broadcast_to(total[b : b + 1, 128 * pair : 128 * pair + 128], (8, 128))
                tile = jnp.where(y == i, row, tile)
            rounds.append(tile)
    logits = jnp.concatenate(rounds, axis=0)
    back = one_hot(iota((128, 128), 1) == (iota((128, 128), 0) & 15) * 8 + (iota((128, 128), 0) >> 4))
    parts = dot(jnp.concatenate(three_terms(logits), axis=0), back)
    logits = (parts[0:32] + parts[32:64] + parts[64:96]).reshape(4, 8, 128)
    result[0] = logits
    out_ref[...] = logits

    pl.when(down)(to_below.wait_send)
    pl.when(up)(to_above.wait_send)
    pl.when(earlier)(to_earlier.wait_send)
    pl.when(later & down)(on_below.wait_send)
    pl.when(later & up)(on_above.wait_send)


def kernel(
    spaces, times, lead,
    ev_hbm, so_hbm, emb_hbm, gain_hbm, cw_hbm, cb_hbm, rw_hbm,
    out_ref,
    ev, so, emb, gain, cw, cb, rw,
    win, unique, ha, hb, final, paired, result,
    load_sem, send_sem, recv_sem, hello,
):
    space, time, core = lax.axis_index("space"), lax.axis_index("tm"), lax.axis_index("chan")
    worker = core == lax.axis_size("chan") - 1
    grid_rows = 8 * spaces
    up, down = space > 0, space < spaces - 1
    later, earlier = time < times - 1, time > 0
    barrier = pltpu.get_barrier_semaphore()

    def remote(src, dst, sent, got, device):
        return pltpu.make_async_remote_copy(
            src_ref=src, dst_ref=dst, send_sem=send_sem.at[sent], recv_sem=recv_sem.at[got],
            device_id=device, device_id_type=MESH,
        )

    def serves(j):
        return space >= j if j == lead else (space >= j) & (space == spaces - 1)

    gives = [
        remote(result.at[j], result.at[0], 5 + lead + j, 5, {"space": space - j, "chan": core - 1}) for j in range(lead + 1)
    ]

    @pl.when(jnp.logical_not(worker))
    def _():
        pl.semaphore_wait(barrier, 1)
        for j in range(lead + 1):
            @pl.when(space + lead <= spaces - 1 if j == lead else space == spaces - 1 - j)
            def _():
                pl.semaphore_signal(
                    hello.at[j], inc=1, device_id={"space": space + j, "chan": core + 1}, device_id_type=MESH
                )
        gives[0].wait_recv()
        out_ref[...] = result[0]

    @pl.when(worker)
    def _():
        loads = [
            pltpu.make_async_copy(src, dst, load_sem.at[i])
            for i, (src, dst) in enumerate(
                ((ev_hbm, ev), (so_hbm, so), (cw_hbm, cw), (emb_hbm, emb), (gain_hbm, gain), (cb_hbm, cb), (rw_hbm, rw))
            )
        ]
        for load in loads:
            load.start()

        def greet(there, device):
            @pl.when(there)
            def _():
                pl.semaphore_signal(barrier, inc=1, device_id=device, device_id_type=MESH)

        greet(up, {"space": space - 1})
        greet(down, {"space": space + 1})
        greet(later, {"tm": time + 1})
        greet(earlier, {"tm": time - 1})
        for j in range(lead + 1):
            greet(serves(j), {"space": space - j, "chan": core - 1})

        compute(
            spaces, space, time, up, down, later, earlier, barrier, grid_rows, remote, loads,
            out_ref, ev, so, emb, gain, cw, cb, rw, win, unique, ha, hb, final, paired, result,
        )

        passes = [remote(result.at[j], result.at[j + 1], 5 + j, 6 + j, {"space": space + 1}) for j in range(lead)]
        for j in range(lead + 1):
            if j > 0:
                pl.when(space >= j)(passes[j - 1].wait_recv)
            if j < lead:
                pl.when(down & (space >= j))(passes[j].start)
        for j in range(lead + 1):
            @pl.when(serves(j))
            def _():
                pl.semaphore_wait(hello.at[j], 1)
                gives[j].start()
        for j in range(lead):
            pl.when(down & (space >= j))(passes[j].wait_send)
        for j in range(lead + 1):
            pl.when(serves(j))(gives[j].wait_send)


def per_device(spaces, times, events, soft_info, embed, soft_gain, conv_weights, conv_bias, readout_weight):
    layers, channels, taps = conv_weights.shape
    gain = soft_gain.reshape(1, channels)
    readout = readout_weight.reshape(1, channels)
    lead = min(LEAD, spaces - 1)
    any_space = pl.BlockSpec(memory_space=pl.ANY)
    return pl.pallas_call(
        functools.partial(kernel, spaces, times, lead),
        out_shape=jax.ShapeDtypeStruct(events.shape, F32),
        in_specs=[any_space] * 7,
        out_specs=pl.BlockSpec(memory_space=pltpu.VMEM),
        scratch_shapes=[
            pltpu.VMEM(events.shape, jnp.int32),
            pltpu.VMEM(soft_info.shape, BF16),
            pltpu.VMEM(embed.shape, F32),
            pltpu.VMEM(gain.shape, F32),
            pltpu.VMEM(conv_weights.shape, BF16),
            pltpu.VMEM(conv_bias.shape, F32),
            pltpu.VMEM(readout.shape, F32),
            pltpu.VMEM((3, 10, 8, 128), BF16),
            pltpu.VMEM((layers, 3, 4, 3, channels, 128), BF16),
            pltpu.VMEM((10, 160, 256), BF16),
            pltpu.VMEM((9, 160, 256), BF16),
            pltpu.VMEM((2, 7, 160, 256), BF16),
            pltpu.VMEM((2, 6, 160, 256), BF16),
            pltpu.VMEM((lead + 1, *events.shape), F32),
            pltpu.SemaphoreType.DMA((7,)),
            pltpu.SemaphoreType.DMA((6 + 2 * lead,)),
            pltpu.SemaphoreType.DMA((6 + lead,)),
            pltpu.SemaphoreType.REGULAR((lead + 1,)),
        ],
        compiler_params=pltpu.CompilerParams(collective_id=0, has_side_effects=True, vmem_limit_bytes=67043328),
    )(events, soft_info, embed, gain, conv_weights, conv_bias, readout)


def solution(mesh):
    tiled = P(("parts", "tm"), "space", None)
    return jax.shard_map(
        functools.partial(per_device, mesh.shape["space"], mesh.shape["tm"]),
        mesh=mesh, in_specs=(tiled, tiled, P(), P(), P(), P(), P()), out_specs=tiled, check_vma=False,
    )
```

```python
import functools

import jax
import jax.numpy as jnp
from jax import lax
from jax.experimental import pallas as pl
from jax.experimental.pallas import tpu as pltpu
from jax.sharding import PartitionSpec as P

F32 = jnp.float32
BF16 = jnp.bfloat16
MESH = pl.DeviceIdType.MESH
LEAD = 3


def iota(shape, dim):
    return lax.broadcasted_iota(jnp.int32, shape, dim)


def three_terms(value):
    high = value.astype(BF16)
    rest = value - high.astype(F32)
    middle = rest.astype(BF16)
    low = (rest - middle.astype(F32)).astype(BF16)
    return high, middle, low


def one_hot(condition):
    return jnp.where(condition, 1.0, 0.0).astype(BF16)


def dot(a, b):
    return lax.dot_general(a, b, (((1,), (0,)), ((), ())), preferred_element_type=F32)


def dot_nt(a, b):
    return lax.dot_general(a, b, (((1,), (1,)), ((), ())), preferred_element_type=F32)


def dot_tn(a, b):
    return lax.dot_general(a, b, (((0,), (0,)), ((), ())), preferred_element_type=F32)


def quad(row):
    return jnp.concatenate([row] * 4, axis=1)


def put(ref, lead, value, count):
    width = value.shape[2]
    q = iota((count, 16, width), 1)
    last, first = value[:, 112:128], value[:, 0:16]
    before = jnp.where(q == 0, 0.0, pltpu.roll(last, 1, 1))
    after = jnp.where(q == 15, 0.0, pltpu.roll(first, 15, 1))
    ref[(*lead, pl.ds(0, count), pl.ds(0, 16))] = before.astype(BF16)
    ref[(*lead, pl.ds(0, count), pl.ds(16, 128))] = value.astype(BF16)
    ref[(*lead, pl.ds(0, count), pl.ds(144, 16))] = after.astype(BF16)


def compute(
    spaces, space, time, up, down, later, earlier, barrier, grid_rows, remote, loads,
    out_ref, ev, so, emb, gain, cw, cb, rw, win, unique, ha, hb, hc, ahead, final, paired, result,
):
    spread = one_hot(iota((128, 128), 0) == (iota((128, 128), 1) & 15) * 8 + (iota((128, 128), 1) >> 4))
    m = iota((64, 64), 0)
    source = (
        (m & 1) * 32 + ((m >> 5) * 2 + 1 - ((m >> 2) & 1)) * 8 + ((m >> 3) & 3) * 2 + ((m >> 1) & 1)
    )
    order = one_hot(iota((64, 64), 1) == source)
    loads[0].wait()
    loads[1].wait()
    raw = jnp.concatenate([ev[...].astype(F32).reshape(32, 128), so[...].astype(F32).reshape(32, 128)], axis=0)
    staged = dot(order, dot(raw.astype(BF16), spread).astype(BF16)).reshape(2, 4, 8, 128).astype(BF16)
    win[0, 3:7] = staged[0]
    win[1, 3:7] = staged[1]

    to_below = remote(win.at[0:2, 4:7], win.at[0:2, 0:3], 0, 0, {"space": space + 1})
    to_above = remote(win.at[0:2, 3:6], win.at[0:2, 7:10], 1, 1, {"space": space - 1})
    to_earlier = remote(win.at[0, 3:7], win.at[2, 3:7], 2, 2, {"tm": time - 1})
    on_below = remote(win.at[2, 4:7], win.at[2, 0:3], 3, 3, {"space": space + 1})
    on_above = remote(win.at[2, 3:6], win.at[2, 7:10], 4, 4, {"space": space - 1})

    pl.semaphore_wait(
        barrier,
        jnp.where(up, 1, 0) + jnp.where(down, 1, 0) + jnp.where(later, 1, 0) + jnp.where(earlier, 1, 0),
    )
    pl.when(down)(to_below.start)
    pl.when(up)(to_above.start)
    pl.when(earlier)(to_earlier.start)

    loads[2].wait()
    blank = jnp.zeros((3, 1, 3, 16, 128), F32)
    for half in range(4):
        pieces = []
        for chunk in (2 * half, 2 * half + 1):
            begin = 216 * chunk // 128 * 128
            stop = min(-(-(216 * chunk + 216) // 128) * 128, cw.shape[2])
            n = iota((216, stop - begin), 0)
            select = one_hot(iota((216, stop - begin), 1) == (n & 7) * 27 + (n >> 3) + (216 * chunk - begin))
            taps = [cw[layer, :, begin:stop] for layer in range(3)]
            two = dot_nt(select, jnp.concatenate([taps[0], taps[0], taps[1], taps[1]], axis=0))
            one = dot_nt(select, jnp.concatenate([taps[2], taps[2]], axis=0))
            pieces.append([v.reshape(27, 8, 128) for v in (two[:, :128], two[:, 128:], one)])
        for layer in range(3):
            tap = jnp.concatenate([pieces[0][layer], pieces[1][layer]], axis=1).reshape(3, 3, 3, 16, 128)
            low = jnp.concatenate([tap, blank], axis=1)
            high = jnp.concatenate([blank, tap], axis=1)
            both = jnp.where(iota((3, 4, 3, 16, 128), 4) < 64, low, high)
            unique[layer, :, :, :, 16 * half : 16 * half + 16, :] = both.astype(BF16)

    for load in loads[3:]:
        load.wait()
    e_terms = three_terms(quad(emb[...]))
    g_terms = three_terms(quad(gain[...]))
    column = jnp.concatenate(
        [t.astype(F32) for t in e_terms] + [t.astype(F32) for t in g_terms] + [jnp.zeros((1, 256), F32)], axis=0
    )
    make = jnp.where(
        iota((64, 256), 0) >> 4 == iota((64, 256), 1) >> 6, jnp.concatenate([column] * 4, axis=0), 0.0
    ).astype(BF16)
    bias = [quad(cb[layer : layer + 1, :]) for layer in range(3)]

    base = 8 * space
    k = iota((16, 128), 0)
    column_parity = iota((16, 128), 1) >> 4

    def inputs(cell, row, there):
        event, signal = cell
        inside = (row >= 0) & (row < grid_rows) & there
        code = 2 * ((column_parity + row) & 1) + event.astype(jnp.int32)
        value = jnp.where(k < 12, jnp.where(code == (k & 3), 1.0, 0.0), jnp.where(k < 15, signal, 0.0))
        return jnp.where(inside, value, 0.0)

    def start(cells, count, first_row, there):
        columns = []
        for j in range(count):
            blocks = []
            for b in range(4):
                blocks.append(inputs(cells(j, b), first_row + 2 * j + (b & 1), there))
            columns.append(jnp.concatenate(blocks, axis=0).astype(BF16))
        return dot_tn(jnp.concatenate(columns, axis=1), make).reshape(count, 128, 256)

    def taps_of(ref, lead, first, count):
        parts = []
        for shift in range(3):
            for pair in range(2):
                part = ref[(*lead, pl.ds(first + pair, count), pl.ds(16 * shift, 128))]
                parts.append(part.reshape(count * 128, part.shape[-1]))
        return parts

    def within(layer):
        rows = []
        for shift in range(3):
            for pair in range(2):
                for r in (1, 0):
                    for y in range(2):
                        rows.append(
                            jnp.concatenate(
                                [unique[layer, r + 1 - to, 2 * pair + y, shift] for to in (1, 0)], axis=1
                            )
                        )
        return jnp.concatenate(rows, axis=0)

    def across(layer):
        rows = []
        none = jnp.zeros((64, 128), BF16)
        for shift in range(3):
            for pair in range(2):
                for y in range(2):
                    rows.append(jnp.concatenate([none, unique[layer, 0, 2 * pair + y, shift]], axis=1))
                for y in range(2):
                    rows.append(jnp.concatenate([unique[layer, 2, 2 * pair + y, shift], none], axis=1))
        return jnp.concatenate(rows, axis=0)

    def finish(total, layer, count, first_row, there):
        row = first_row + 2 * iota((count, 1, 256), 0) + ((iota((count, 1, 256), 2) >> 6) & 1)
        inside = (row >= 0) & (row < grid_rows) & there
        value = jnp.maximum(total + bias[layer], 0.0).reshape(count, 128, 256)
        return value * jnp.where(inside, 1.0, 0.0)

    pl.when(later)(to_earlier.wait_recv)
    pl.when(later & down)(on_below.start)
    pl.when(later & up)(on_above.start)
    pl.when(up)(to_below.wait_recv)
    pl.when(down)(to_above.wait_recv)

    pl.when(later & up)(on_below.wait_recv)
    pl.when(later & down)(on_above.wait_recv)
    for w, there in ((0, True), (1, later)):
        def cells(j, b):
            tile = win[2 * w, j].astype(F32)
            return tile[2 * b : 2 * b + 1], tile[2 * b + 1 : 2 * b + 2]

        put(ha, (w,), start(cells, 10, base - 6, there), 10)
    for w, there in ((0, True), (1, later)):
        total = dot(jnp.concatenate(taps_of(ha, (w,), 0, 9), axis=1), within(0))
        put(hb, (w,), finish(total, 0, 9, base - 5, there), 9)
    for w, there in ((0, True), (1, later)):
        total = dot(jnp.concatenate(taps_of(hb, (w,), 0, 8), axis=1), within(1))
        put(hc, (w,), finish(total, 1, 8, base - 4, there), 8)
    for w, there in ((0, True), (1, later)):
        total = dot(jnp.concatenate(taps_of(hc, (w,), 0, 7), axis=1), within(2))
        value = finish(total, 2, 7, base - 3, there)
        half = 128 * w
        put(final, (w,), value[:, :, half : half + 128], 7)
        swapped = jnp.where((iota((6, 128, 128), 2) & 64) == 0, value[1:7, :, half : half + 128], value[0:6, :, half : half + 128])
        put(paired, (w,), pltpu.roll(swapped, 64, 2), 6)
        if w == 0:
            ahead[...] = value[1:6, :, 128:256].astype(BF16)

    def beside(ref, first, count):
        left = taps_of(ref, (0,), first, count)
        right = taps_of(ref, (1,), first, count)
        return [v for pair in zip(left, right) for v in pair]

    def second(own, others, layer, count, first_other):
        lhs = jnp.concatenate(taps_of(own, (0,), 0, count) + beside(others, first_other, count), axis=1)
        return dot(lhs, jnp.concatenate([within(layer), across(layer)], axis=0))

    def late_cells(j, b):
        tile = win[1, 1 + j + (b & 1)].astype(F32)
        at = (b >> 1) * 4 + (1 - (b & 1)) * 2
        return tile[at : at + 1], tile[at + 1 : at + 2]

    put(ha, (0,), start(late_cells, 7, base - 3, True), 7)
    put(hb, (0,), finish(second(ha, final, 0, 6, 0), 0, 6, base - 2, True), 6)
    put(hc, (0,), finish(second(hb, paired, 1, 5, 0), 1, 5, base - 1, True), 5)
    last = finish(second(hc, final, 2, 4, 1), 2, 4, base, True).astype(BF16).reshape(512, 256)

    w_terms = three_terms(quad(rw[...]))
    n = iota((32, 256), 0)
    weight = jnp.where(n >> 3 == 0, w_terms[0].astype(F32), jnp.where(n >> 3 == 1, w_terms[1].astype(F32), w_terms[2].astype(F32)))
    weight = jnp.where((n < 24) & ((n & 7) == iota((32, 256), 1) >> 6), weight, 0.0).astype(BF16)
    first = jnp.concatenate([final[0, 1:6, 16:144, :].reshape(640, 128), ahead[...].reshape(640, 128)], axis=1)
    a_sum = dot_nt(weight, first)
    b_sum = dot_nt(weight, last)
    a_sum = a_sum[0:8] + a_sum[8:16] + a_sum[16:24]
    b_sum = b_sum[0:8] + b_sum[8:16] + b_sum[16:24]
    y = iota((8, 128), 0)
    rounds = []
    for total, shift in ((a_sum, 1), (b_sum, 0)):
        for r in range(2):
            tile = jnp.zeros((8, 128), F32)
            for i in range(8):
                pair, inner = (i + shift) // 2, (i + shift) % 2
                b = (1 - r) * 2 + inner
                row = jnp.broadcast_to(total[b : b + 1, 128 * pair : 128 * pair + 128], (8, 128))
                tile = jnp.where(y == i, row, tile)
            rounds.append(tile)
    logits = jnp.concatenate(rounds, axis=0)
    back = one_hot(iota((128, 128), 1) == (iota((128, 128), 0) & 15) * 8 + (iota((128, 128), 0) >> 4))
    parts = dot(jnp.concatenate(three_terms(logits), axis=0), back)
    logits = (parts[0:32] + parts[32:64] + parts[64:96]).reshape(4, 8, 128)
    result[0] = logits
    out_ref[...] = logits

    pl.when(down)(to_below.wait_send)
    pl.when(up)(to_above.wait_send)
    pl.when(earlier)(to_earlier.wait_send)
    pl.when(later & down)(on_below.wait_send)
    pl.when(later & up)(on_above.wait_send)


def kernel(
    spaces, times, lead,
    ev_hbm, so_hbm, emb_hbm, gain_hbm, cw_hbm, cb_hbm, rw_hbm,
    out_ref,
    ev, so, emb, gain, cw, cb, rw,
    win, unique, ha, hb, hc, ahead, final, paired, result,
    load_sem, send_sem, recv_sem, hello,
):
    space, time, core = lax.axis_index("space"), lax.axis_index("tm"), lax.axis_index("chan")
    worker = core == lax.axis_size("chan") - 1
    grid_rows = 8 * spaces
    up, down = space > 0, space < spaces - 1
    later, earlier = time < times - 1, time > 0
    barrier = pltpu.get_barrier_semaphore()

    def remote(src, dst, sent, got, device):
        return pltpu.make_async_remote_copy(
            src_ref=src, dst_ref=dst, send_sem=send_sem.at[sent], recv_sem=recv_sem.at[got],
            device_id=device, device_id_type=MESH,
        )

    def serves(j):
        return space >= j if j == lead else (space >= j) & (space == spaces - 1)

    gives = [
        remote(result.at[j], result.at[0], 5 + lead + j, 5, {"space": space - j, "chan": core - 1}) for j in range(lead + 1)
    ]

    @pl.when(jnp.logical_not(worker))
    def _():
        pl.semaphore_wait(barrier, 1)
        for j in range(lead + 1):
            @pl.when(space + lead <= spaces - 1 if j == lead else space == spaces - 1 - j)
            def _():
                pl.semaphore_signal(
                    hello.at[j], inc=1, device_id={"space": space + j, "chan": core + 1}, device_id_type=MESH
                )
        gives[0].wait_recv()
        out_ref[...] = result[0]

    @pl.when(worker)
    def _():
        loads = [
            pltpu.make_async_copy(src, dst, load_sem.at[i])
            for i, (src, dst) in enumerate(
                ((ev_hbm, ev), (so_hbm, so), (cw_hbm, cw), (emb_hbm, emb), (gain_hbm, gain), (cb_hbm, cb), (rw_hbm, rw))
            )
        ]
        for load in loads:
            load.start()

        def greet(there, device):
            @pl.when(there)
            def _():
                pl.semaphore_signal(barrier, inc=1, device_id=device, device_id_type=MESH)

        greet(up, {"space": space - 1})
        greet(down, {"space": space + 1})
        greet(later, {"tm": time + 1})
        greet(earlier, {"tm": time - 1})
        for j in range(lead + 1):
            greet(serves(j), {"space": space - j, "chan": core - 1})

        compute(
            spaces, space, time, up, down, later, earlier, barrier, grid_rows, remote, loads,
            out_ref, ev, so, emb, gain, cw, cb, rw, win, unique, ha, hb, hc, ahead, final, paired, result,
        )

        passes = [remote(result.at[j], result.at[j + 1], 5 + j, 6 + j, {"space": space + 1}) for j in range(lead)]
        for j in range(lead + 1):
            if j > 0:
                pl.when(space >= j)(passes[j - 1].wait_recv)
            if j < lead:
                pl.when(down & (space >= j))(passes[j].start)
        for j in range(lead + 1):
            @pl.when(serves(j))
            def _():
                pl.semaphore_wait(hello.at[j], 1)
                gives[j].start()
        for j in range(lead):
            pl.when(down & (space >= j))(passes[j].wait_send)
        for j in range(lead + 1):
            pl.when(serves(j))(gives[j].wait_send)


def per_device(spaces, times, events, soft_info, embed, soft_gain, conv_weights, conv_bias, readout_weight):
    layers, channels, taps = conv_weights.shape
    gain = soft_gain.reshape(1, channels)
    readout = readout_weight.reshape(1, channels)
    lead = min(LEAD, spaces - 1)
    any_space = pl.BlockSpec(memory_space=pl.ANY)
    return pl.pallas_call(
        functools.partial(kernel, spaces, times, lead),
        out_shape=jax.ShapeDtypeStruct(events.shape, F32),
        in_specs=[any_space] * 7,
        out_specs=pl.BlockSpec(memory_space=pltpu.VMEM),
        scratch_shapes=[
            pltpu.VMEM(events.shape, jnp.int32),
            pltpu.VMEM(soft_info.shape, BF16),
            pltpu.VMEM(embed.shape, F32),
            pltpu.VMEM(gain.shape, F32),
            pltpu.VMEM(conv_weights.shape, BF16),
            pltpu.VMEM(conv_bias.shape, F32),
            pltpu.VMEM(readout.shape, F32),
            pltpu.VMEM((3, 10, 8, 128), BF16),
            pltpu.VMEM((layers, 3, 4, 3, channels, 128), BF16),
            pltpu.VMEM((2, 10, 160, 256), BF16),
            pltpu.VMEM((2, 9, 160, 256), BF16),
            pltpu.VMEM((2, 8, 160, 256), BF16),
            pltpu.VMEM((5, 128, 128), BF16),
            pltpu.VMEM((2, 7, 160, 128), BF16),
            pltpu.VMEM((2, 6, 160, 128), BF16),
            pltpu.VMEM((lead + 1, *events.shape), F32),
            pltpu.SemaphoreType.DMA((7,)),
            pltpu.SemaphoreType.DMA((6 + 2 * lead,)),
            pltpu.SemaphoreType.DMA((6 + lead,)),
            pltpu.SemaphoreType.REGULAR((lead + 1,)),
        ],
        compiler_params=pltpu.CompilerParams(collective_id=0, has_side_effects=True, vmem_limit_bytes=48 * 1024 * 1024),
    )(*[pltpu.with_memory_space_constraint(v, pltpu.HBM) for v in (events, soft_info, embed, gain, conv_weights, conv_bias, readout)])


def solution(mesh):
    tiled = P(("parts", "tm"), "space", None)
    return jax.shard_map(
        functools.partial(per_device, mesh.shape["space"], mesh.shape["tm"]),
        mesh=mesh, in_specs=(tiled, tiled, P(), P(), P(), P(), P()), out_specs=tiled, check_vma=False,
    )
```

```python
import functools

import jax
import jax.numpy as jnp
from jax import lax
from jax.experimental import pallas as pl
from jax.experimental.pallas import tpu as pltpu
from jax.sharding import PartitionSpec as P

F32 = jnp.float32
BF16 = jnp.bfloat16
MESH = pl.DeviceIdType.MESH
LEAD = 4


def iota(shape, dim):
    return lax.broadcasted_iota(jnp.int32, shape, dim)


def three_terms(value):
    high = value.astype(BF16)
    rest = value - high.astype(F32)
    middle = rest.astype(BF16)
    low = (rest - middle.astype(F32)).astype(BF16)
    return high, middle, low


def one_hot(condition):
    return jnp.where(condition, 1.0, 0.0).astype(BF16)


def dot(a, b):
    return lax.dot_general(a, b, (((1,), (0,)), ((), ())), preferred_element_type=F32)


def dot_nt(a, b):
    return lax.dot_general(a, b, (((1,), (1,)), ((), ())), preferred_element_type=F32)


def dot_tn(a, b):
    return lax.dot_general(a, b, (((0,), (0,)), ((), ())), preferred_element_type=F32)


def quad(row):
    return jnp.concatenate([row] * 4, axis=1)


def put(ref, lead, value, first, count):
    width = value.shape[2]
    q = iota((count, 16, width), 1)
    last, head = value[:, 112:128], value[:, 0:16]
    before = jnp.where(q == 0, 0.0, pltpu.roll(last, 1, 1))
    after = jnp.where(q == 15, 0.0, pltpu.roll(head, 15, 1))
    ref[(*lead, pl.ds(first, count), pl.ds(0, 16))] = before.astype(BF16)
    ref[(*lead, pl.ds(first, count), pl.ds(16, 128))] = value.astype(BF16)
    ref[(*lead, pl.ds(first, count), pl.ds(144, 16))] = after.astype(BF16)


def compute(
    spaces, space, time, up, down, later, earlier, barrier, ready, grid_rows, remote, loads,
    out_ref, ev, so, emb, gain, cw, cb, rw, win, unique, ha, hb, hc, ahead, final, paired, result,
):
    spread = one_hot(iota((128, 128), 0) == (iota((128, 128), 1) & 15) * 8 + (iota((128, 128), 1) >> 4))
    m = iota((64, 64), 0)
    source = (
        (m & 1) * 32 + ((m >> 5) * 2 + 1 - ((m >> 2) & 1)) * 8 + ((m >> 3) & 3) * 2 + ((m >> 1) & 1)
    )
    order = one_hot(iota((64, 64), 1) == source)
    loads[0].wait()
    loads[1].wait()
    raw = jnp.concatenate([ev[...].astype(F32).reshape(32, 128), so[...].astype(F32).reshape(32, 128)], axis=0)
    staged = dot(order, dot(raw.astype(BF16), spread).astype(BF16)).reshape(2, 4, 8, 128).astype(BF16)
    win[0, 3:7] = staged[0]
    win[1, 3:7] = staged[1]

    to_below = remote(win.at[0:2, 4:7], win.at[0:2, 0:3], 0, 0, {"space": space + 1})
    to_above = remote(win.at[0:2, 3:6], win.at[0:2, 7:10], 1, 1, {"space": space - 1})
    to_earlier = remote(win.at[0, 3:7], win.at[2, 3:7], 2, 2, {"tm": time - 1})
    on_below = remote(win.at[2, 4:7], win.at[2, 0:3], 3, 3, {"space": space + 1})
    to_corner = remote(win.at[0, 3:6], win.at[2, 7:10], 4, 4, {"space": space - 1, "tm": time - 1})

    pl.semaphore_wait(
        barrier,
        jnp.where(up, 1, 0) + jnp.where(later, 1, 0) + jnp.where(earlier, 1, 0) + jnp.where(up & earlier, 1, 0),
    )
    pl.when(up)(to_above.start)
    pl.when(up & earlier)(to_corner.start)
    pl.when(earlier)(to_earlier.start)

    @pl.when(up)
    def _():
        pl.semaphore_signal(ready, inc=1, device_id={"space": space - 1}, device_id_type=MESH)

    loads[2].wait()
    blank = jnp.zeros((3, 1, 3, 16, 128), F32)
    for half in range(4):
        pieces = []
        for chunk in (2 * half, 2 * half + 1):
            begin = 216 * chunk // 128 * 128
            stop = min(-(-(216 * chunk + 216) // 128) * 128, cw.shape[2])
            n = iota((216, stop - begin), 0)
            select = one_hot(iota((216, stop - begin), 1) == (n & 7) * 27 + (n >> 3) + (216 * chunk - begin))
            taps = [cw[layer, :, begin:stop] for layer in range(3)]
            two = dot_nt(select, jnp.concatenate([taps[0], taps[0], taps[1], taps[1]], axis=0))
            one = dot_nt(select, jnp.concatenate([taps[2], taps[2]], axis=0))
            pieces.append([v.reshape(27, 8, 128) for v in (two[:, :128], two[:, 128:], one)])
        for layer in range(3):
            tap = jnp.concatenate([pieces[0][layer], pieces[1][layer]], axis=1).reshape(3, 3, 3, 16, 128)
            low = jnp.concatenate([tap, blank], axis=1)
            high = jnp.concatenate([blank, tap], axis=1)
            both = jnp.where(iota((3, 4, 3, 16, 128), 4) < 64, low, high)
            unique[layer, :, :, :, 16 * half : 16 * half + 16, :] = both.astype(BF16)

    for load in loads[3:]:
        load.wait()
    e_terms = three_terms(quad(emb[...]))
    g_terms = three_terms(quad(gain[...]))
    column = jnp.concatenate(
        [t.astype(F32) for t in e_terms] + [t.astype(F32) for t in g_terms] + [jnp.zeros((1, 256), F32)], axis=0
    )
    make = jnp.where(
        iota((64, 256), 0) >> 4 == iota((64, 256), 1) >> 6, jnp.concatenate([column] * 4, axis=0), 0.0
    ).astype(BF16)
    bias = [quad(cb[layer : layer + 1, :]) for layer in range(3)]

    base = 8 * space
    k = iota((16, 128), 0)
    column_parity = iota((16, 128), 1) >> 4

    def inputs(cell, row, there):
        event, signal = cell
        inside = (row >= 0) & (row < grid_rows) & there
        code = 2 * ((column_parity + row) & 1) + event.astype(jnp.int32)
        value = jnp.where(k < 12, jnp.where(code == (k & 3), 1.0, 0.0), jnp.where(k < 15, signal, 0.0))
        return jnp.where(inside, value, 0.0)

    def start(cells, first, count, first_row, there):
        columns = []
        for j in range(first, first + count):
            blocks = []
            for b in range(4):
                blocks.append(inputs(cells(j, b), first_row + 2 * j + (b & 1), there))
            columns.append(jnp.concatenate(blocks, axis=0).astype(BF16))
        return dot_tn(jnp.concatenate(columns, axis=1), make).reshape(count, 128, 256)

    def taps_of(ref, lead, first, count):
        parts = []
        for shift in range(3):
            for pair in range(2):
                part = ref[(*lead, pl.ds(first + pair, count), pl.ds(16 * shift, 128))]
                parts.append(part.reshape(count * 128, part.shape[-1]))
        return parts

    def within(layer):
        rows = []
        for shift in range(3):
            for pair in range(2):
                for r in (1, 0):
                    for y in range(2):
                        rows.append(
                            jnp.concatenate(
                                [unique[layer, r + 1 - to, 2 * pair + y, shift] for to in (1, 0)], axis=1
                            )
                        )
        return jnp.concatenate(rows, axis=0)

    def across(layer):
        rows = []
        none = jnp.zeros((64, 128), BF16)
        for shift in range(3):
            for pair in range(2):
                for y in range(2):
                    rows.append(jnp.concatenate([none, unique[layer, 0, 2 * pair + y, shift]], axis=1))
                for y in range(2):
                    rows.append(jnp.concatenate([unique[layer, 2, 2 * pair + y, shift], none], axis=1))
        return jnp.concatenate(rows, axis=0)

    def finish(total, layer, count, first_row, there):
        row = first_row + 2 * iota((count, 1, 256), 0) + ((iota((count, 1, 256), 2) >> 6) & 1)
        inside = (row >= 0) & (row < grid_rows) & there
        value = jnp.maximum(total + bias[layer], 0.0).reshape(count, 128, 256)
        return value * jnp.where(inside, 1.0, 0.0)

    windows = ((0, True), (1, later))

    def begin(w, there, first, count):
        def cells(j, b):
            tile = win[2 * w, j].astype(F32)
            return tile[2 * b : 2 * b + 1], tile[2 * b + 1 : 2 * b + 2]

        put(ha, (w,), start(cells, first, count, base - 6, there), first, count)

    def first_layer(w, there, first, count):
        total = dot(jnp.concatenate(taps_of(ha, (w,), first, count), axis=1), within(0))
        put(hb, (w,), finish(total, 0, count, base - 5 + 2 * first, there), first, count)

    pl.when(later)(to_earlier.wait_recv)
    for w, there in windows:
        begin(w, there, 3, 4)

    @pl.when(down)
    def _():
        pl.semaphore_wait(ready, 1)
        to_below.start()

    pl.when(down & later)(on_below.start)
    pl.when(up)(to_below.wait_recv)
    pl.when(up & later)(on_below.wait_recv)
    for w, there in windows:
        begin(w, there, 0, 3)
    for w, there in windows:
        first_layer(w, there, 0, 6)
    pl.when(down)(to_above.wait_recv)
    pl.when(down & later)(to_corner.wait_recv)
    for w, there in windows:
        begin(w, there, 7, 3)
    for w, there in windows:
        first_layer(w, there, 6, 3)
    for w, there in ((0, True), (1, later)):
        total = dot(jnp.concatenate(taps_of(hb, (w,), 0, 8), axis=1), within(1))
        put(hc, (w,), finish(total, 1, 8, base - 4, there), 0, 8)
    for w, there in ((0, True), (1, later)):
        total = dot(jnp.concatenate(taps_of(hc, (w,), 0, 7), axis=1), within(2))
        value = finish(total, 2, 7, base - 3, there)
        half = 128 * w
        put(final, (w,), value[:, :, half : half + 128], 0, 7)
        swapped = jnp.where((iota((6, 128, 128), 2) & 64) == 0, value[1:7, :, half : half + 128], value[0:6, :, half : half + 128])
        put(paired, (w,), pltpu.roll(swapped, 64, 2), 0, 6)
        if w == 0:
            ahead[...] = value[1:6, :, 128:256].astype(BF16)

    def beside(ref, first, count):
        left = taps_of(ref, (0,), first, count)
        right = taps_of(ref, (1,), first, count)
        return [v for pair in zip(left, right) for v in pair]

    def second(own, others, layer, count, first_other):
        lhs = jnp.concatenate(taps_of(own, (0,), 0, count) + beside(others, first_other, count), axis=1)
        return dot(lhs, jnp.concatenate([within(layer), across(layer)], axis=0))

    def late_cells(j, b):
        tile = win[1, 1 + j + (b & 1)].astype(F32)
        at = (b >> 1) * 4 + (1 - (b & 1)) * 2
        return tile[at : at + 1], tile[at + 1 : at + 2]

    put(ha, (0,), start(late_cells, 0, 7, base - 3, True), 0, 7)
    put(hb, (0,), finish(second(ha, final, 0, 6, 0), 0, 6, base - 2, True), 0, 6)
    put(hc, (0,), finish(second(hb, paired, 1, 5, 0), 1, 5, base - 1, True), 0, 5)
    last = finish(second(hc, final, 2, 4, 1), 2, 4, base, True).astype(BF16).reshape(512, 256)

    w_terms = three_terms(quad(rw[...]))
    n = iota((32, 256), 0)
    weight = jnp.where(n >> 3 == 0, w_terms[0].astype(F32), jnp.where(n >> 3 == 1, w_terms[1].astype(F32), w_terms[2].astype(F32)))
    weight = jnp.where((n < 24) & ((n & 7) == iota((32, 256), 1) >> 6), weight, 0.0).astype(BF16)
    first = jnp.concatenate([final[0, 1:6, 16:144, :].reshape(640, 128), ahead[...].reshape(640, 128)], axis=1)
    a_sum = dot_nt(weight, first)
    b_sum = dot_nt(weight, last)
    a_sum = a_sum[0:8] + a_sum[8:16] + a_sum[16:24]
    b_sum = b_sum[0:8] + b_sum[8:16] + b_sum[16:24]
    y = iota((8, 128), 0)
    rounds = []
    for total, shift in ((a_sum, 1), (b_sum, 0)):
        for r in range(2):
            tile = jnp.zeros((8, 128), F32)
            for i in range(8):
                pair, inner = (i + shift) // 2, (i + shift) % 2
                b = (1 - r) * 2 + inner
                row = jnp.broadcast_to(total[b : b + 1, 128 * pair : 128 * pair + 128], (8, 128))
                tile = jnp.where(y == i, row, tile)
            rounds.append(tile)
    logits = jnp.concatenate(rounds, axis=0)
    back = one_hot(iota((128, 128), 1) == (iota((128, 128), 0) & 15) * 8 + (iota((128, 128), 0) >> 4))
    parts = dot(jnp.concatenate(three_terms(logits), axis=0), back)
    logits = (parts[0:32] + parts[32:64] + parts[64:96]).reshape(4, 8, 128)
    result[0] = logits
    out_ref[...] = logits

    pl.when(down)(to_below.wait_send)
    pl.when(up)(to_above.wait_send)
    pl.when(earlier)(to_earlier.wait_send)
    pl.when(later & down)(on_below.wait_send)
    pl.when(up & earlier)(to_corner.wait_send)


def kernel(
    spaces, times, lead,
    ev_hbm, so_hbm, emb_hbm, gain_hbm, cw_hbm, cb_hbm, rw_hbm,
    out_ref,
    ev, so, emb, gain, cw, cb, rw,
    win, unique, ha, hb, hc, ahead, final, paired, result,
    load_sem, send_sem, recv_sem, hello, ready,
):
    space, time, core = lax.axis_index("space"), lax.axis_index("tm"), lax.axis_index("chan")
    worker = core == lax.axis_size("chan") - 1
    grid_rows = 8 * spaces
    up, down = space > 0, space < spaces - 1
    later, earlier = time < times - 1, time > 0
    barrier = pltpu.get_barrier_semaphore()

    def remote(src, dst, sent, got, device):
        return pltpu.make_async_remote_copy(
            src_ref=src, dst_ref=dst, send_sem=send_sem.at[sent], recv_sem=recv_sem.at[got],
            device_id=device, device_id_type=MESH,
        )

    def serves(j):
        return space >= j if j == lead else (space >= j) & (space == spaces - 1)

    gives = [
        remote(result.at[j], result.at[0], 5 + lead + j, 5, {"space": space - j, "chan": core - 1}) for j in range(lead + 1)
    ]

    @pl.when(jnp.logical_not(worker))
    def _():
        pl.semaphore_wait(barrier, 1)
        for j in range(lead + 1):
            @pl.when(space + lead <= spaces - 1 if j == lead else space == spaces - 1 - j)
            def _():
                pl.semaphore_signal(
                    hello.at[j], inc=1, device_id={"space": space + j, "chan": core + 1}, device_id_type=MESH
                )
        gives[0].wait_recv()
        out_ref[...] = result[0]

    @pl.when(worker)
    def _():
        loads = [
            pltpu.make_async_copy(src, dst, load_sem.at[i])
            for i, (src, dst) in enumerate(
                ((ev_hbm, ev), (so_hbm, so), (cw_hbm, cw), (emb_hbm, emb), (gain_hbm, gain), (cb_hbm, cb), (rw_hbm, rw))
            )
        ]
        for load in loads:
            load.start()

        def greet(there, device):
            @pl.when(there)
            def _():
                pl.semaphore_signal(barrier, inc=1, device_id=device, device_id_type=MESH)

        greet(down, {"space": space + 1})
        greet(later, {"tm": time + 1})
        greet(earlier, {"tm": time - 1})
        greet(down & later, {"space": space + 1, "tm": time + 1})
        for j in range(lead + 1):
            greet(serves(j), {"space": space - j, "chan": core - 1})

        compute(
            spaces, space, time, up, down, later, earlier, barrier, ready, grid_rows, remote, loads,
            out_ref, ev, so, emb, gain, cw, cb, rw, win, unique, ha, hb, hc, ahead, final, paired, result,
        )

        passes = [remote(result.at[j], result.at[j + 1], 5 + j, 6 + j, {"space": space + 1}) for j in range(lead)]
        for j in range(lead + 1):
            if j > 0:
                pl.when(space >= j)(passes[j - 1].wait_recv)
            if j < lead:
                pl.when(down & (space >= j))(passes[j].start)
        for j in range(lead + 1):
            @pl.when(serves(j))
            def _():
                pl.semaphore_wait(hello.at[j], 1)
                gives[j].start()
        for j in range(lead):
            pl.when(down & (space >= j))(passes[j].wait_send)
        for j in range(lead + 1):
            pl.when(serves(j))(gives[j].wait_send)


def per_device(spaces, times, events, soft_info, embed, soft_gain, conv_weights, conv_bias, readout_weight):
    layers, channels, taps = conv_weights.shape
    gain = soft_gain.reshape(1, channels)
    readout = readout_weight.reshape(1, channels)
    lead = min(LEAD, spaces - 1)
    any_space = pl.BlockSpec(memory_space=pl.ANY)
    return pl.pallas_call(
        functools.partial(kernel, spaces, times, lead),
        out_shape=jax.ShapeDtypeStruct(events.shape, F32),
        in_specs=[any_space] * 7,
        out_specs=pl.BlockSpec(memory_space=pltpu.VMEM),
        scratch_shapes=[
            pltpu.VMEM(events.shape, jnp.int32),
            pltpu.VMEM(soft_info.shape, BF16),
            pltpu.VMEM(embed.shape, F32),
            pltpu.VMEM(gain.shape, F32),
            pltpu.VMEM(conv_weights.shape, BF16),
            pltpu.VMEM(conv_bias.shape, F32),
            pltpu.VMEM(readout.shape, F32),
            pltpu.VMEM((3, 10, 8, 128), BF16),
            pltpu.VMEM((layers, 3, 4, 3, channels, 128), BF16),
            pltpu.VMEM((2, 10, 160, 256), BF16),
            pltpu.VMEM((2, 9, 160, 256), BF16),
            pltpu.VMEM((2, 8, 160, 256), BF16),
            pltpu.VMEM((5, 128, 128), BF16),
            pltpu.VMEM((2, 7, 160, 128), BF16),
            pltpu.VMEM((2, 6, 160, 128), BF16),
            pltpu.VMEM((lead + 1, *events.shape), F32),
            pltpu.SemaphoreType.DMA((7,)),
            pltpu.SemaphoreType.DMA((6 + 2 * lead,)),
            pltpu.SemaphoreType.DMA((6 + lead,)),
            pltpu.SemaphoreType.REGULAR((lead + 1,)),
            pltpu.SemaphoreType.REGULAR,
        ],
        compiler_params=pltpu.CompilerParams(collective_id=0, has_side_effects=True, vmem_limit_bytes=48 * 1024 * 1024),
    )(*[pltpu.with_memory_space_constraint(v, pltpu.HBM) for v in (events, soft_info, embed, gain, conv_weights, conv_bias, readout)])


def solution(mesh):
    tiled = P(("parts", "tm"), "space", None)
    return jax.shard_map(
        functools.partial(per_device, mesh.shape["space"], mesh.shape["tm"]),
        mesh=mesh, in_specs=(tiled, tiled, P(), P(), P(), P(), P()), out_specs=tiled, check_vma=False,
    )
```

```python
import functools

import jax
import jax.numpy as jnp
from jax import lax
from jax.experimental import pallas as pl
from jax.experimental.pallas import tpu as pltpu
from jax.sharding import PartitionSpec as P

F32 = jnp.float32
BF16 = jnp.bfloat16
MESH = pl.DeviceIdType.MESH
LEAD = 3


def iota(shape, dim):
    return lax.broadcasted_iota(jnp.int32, shape, dim)


def three_terms(value):
    high = value.astype(BF16)
    rest = value - high.astype(F32)
    middle = rest.astype(BF16)
    low = (rest - middle.astype(F32)).astype(BF16)
    return high, middle, low


def one_hot(condition):
    return jnp.where(condition, 1.0, 0.0).astype(BF16)


def dot(a, b):
    return lax.dot_general(a, b, (((1,), (0,)), ((), ())), preferred_element_type=F32)


def dot_nt(a, b):
    return lax.dot_general(a, b, (((1,), (1,)), ((), ())), preferred_element_type=F32)


def dot_tn(a, b):
    return lax.dot_general(a, b, (((0,), (0,)), ((), ())), preferred_element_type=F32)


def quad(row):
    return jnp.concatenate([row] * 4, axis=1)


def put(ref, lead, value, first, count):
    width = value.shape[2]
    q = iota((count, 16, width), 1)
    last, head = value[:, 112:128], value[:, 0:16]
    before = jnp.where(q == 0, 0.0, pltpu.roll(last, 1, 1))
    after = jnp.where(q == 15, 0.0, pltpu.roll(head, 15, 1))
    ref[(*lead, pl.ds(first, count), pl.ds(0, 16))] = before.astype(BF16)
    ref[(*lead, pl.ds(first, count), pl.ds(16, 128))] = value.astype(BF16)
    ref[(*lead, pl.ds(first, count), pl.ds(144, 16))] = after.astype(BF16)


def compute(
    spaces, space, time, up, down, later, earlier, barrier, ready, grid_rows, remote, loads,
    out_ref, ev, so, emb, gain, cw, cb, rw, win, unique, ha, hb, hc, hd, ahead, final, paired, result,
):
    spread = one_hot(iota((128, 128), 0) == (iota((128, 128), 1) & 15) * 8 + (iota((128, 128), 1) >> 4))
    m = iota((64, 64), 0)
    source = (
        (m & 1) * 32 + ((m >> 5) * 2 + 1 - ((m >> 2) & 1)) * 8 + ((m >> 3) & 3) * 2 + ((m >> 1) & 1)
    )
    order = one_hot(iota((64, 64), 1) == source)
    loads[0].wait()
    loads[1].wait()
    raw = jnp.concatenate([ev[...].astype(F32).reshape(32, 128), so[...].astype(F32).reshape(32, 128)], axis=0)
    staged = dot(order, dot(raw.astype(BF16), spread).astype(BF16)).reshape(2, 4, 8, 128).astype(BF16)
    win[0, 3:7] = staged[0]
    win[1, 3:7] = staged[1]

    to_below = remote(win.at[0:2, 4:7], win.at[0:2, 0:3], 0, 0, {"space": space + 1})
    to_above = remote(win.at[0:2, 3:6], win.at[0:2, 7:10], 1, 1, {"space": space - 1})
    to_earlier = remote(win.at[0, 3:7], win.at[2, 3:7], 2, 2, {"tm": time - 1})
    on_below = remote(win.at[2, 4:7], win.at[2, 0:3], 3, 3, {"space": space + 1})
    to_corner = remote(win.at[0, 3:6], win.at[2, 7:10], 4, 4, {"space": space - 1, "tm": time - 1})

    pl.semaphore_wait(
        barrier,
        jnp.where(up, 1, 0) + jnp.where(later, 1, 0) + jnp.where(earlier, 1, 0) + jnp.where(up & earlier, 1, 0),
    )
    pl.when(up)(to_above.start)
    pl.when(up & earlier)(to_corner.start)
    pl.when(earlier)(to_earlier.start)

    @pl.when(up)
    def _():
        pl.semaphore_signal(ready, inc=1, device_id={"space": space - 1}, device_id_type=MESH)

    loads[2].wait()
    blank = jnp.zeros((3, 1, 3, 16, 128), F32)
    for half in range(4):
        pieces = []
        for chunk in (2 * half, 2 * half + 1):
            begin = 216 * chunk // 128 * 128
            stop = min(-(-(216 * chunk + 216) // 128) * 128, cw.shape[2])
            n = iota((216, stop - begin), 0)
            select = one_hot(iota((216, stop - begin), 1) == (n & 7) * 27 + (n >> 3) + (216 * chunk - begin))
            taps = [cw[layer, :, begin:stop] for layer in range(3)]
            two = dot_nt(select, jnp.concatenate([taps[0], taps[0], taps[1], taps[1]], axis=0))
            one = dot_nt(select, jnp.concatenate([taps[2], taps[2]], axis=0))
            pieces.append([v.reshape(27, 8, 128) for v in (two[:, :128], two[:, 128:], one)])
        for layer in range(3):
            tap = jnp.concatenate([pieces[0][layer], pieces[1][layer]], axis=1).reshape(3, 3, 3, 16, 128)
            low = jnp.concatenate([tap, blank], axis=1)
            high = jnp.concatenate([blank, tap], axis=1)
            both = jnp.where(iota((3, 4, 3, 16, 128), 4) < 64, low, high)
            unique[layer, :, :, :, 16 * half : 16 * half + 16, :] = both.astype(BF16)

    for load in loads[3:]:
        load.wait()
    e_terms = three_terms(quad(emb[...]))
    g_terms = three_terms(quad(gain[...]))
    column = jnp.concatenate(
        [t.astype(F32) for t in e_terms] + [t.astype(F32) for t in g_terms] + [jnp.zeros((1, 256), F32)], axis=0
    )
    make = jnp.where(
        iota((64, 256), 0) >> 4 == iota((64, 256), 1) >> 6, jnp.concatenate([column] * 4, axis=0), 0.0
    ).astype(BF16)
    bias = [quad(cb[layer : layer + 1, :]) for layer in range(3)]

    base = 8 * space
    k = iota((16, 128), 0)
    column_parity = iota((16, 128), 1) >> 4

    def inputs(cell, row, there):
        event, signal = cell
        inside = (row >= 0) & (row < grid_rows) & there
        code = 2 * ((column_parity + row) & 1) + event.astype(jnp.int32)
        value = jnp.where(k < 12, jnp.where(code == (k & 3), 1.0, 0.0), jnp.where(k < 15, signal, 0.0))
        return jnp.where(inside, value, 0.0)

    def start(cells, first, count, first_row, there):
        columns = []
        for j in range(first, first + count):
            blocks = []
            for b in range(4):
                blocks.append(inputs(cells(j, b), first_row + 2 * j + (b & 1), there))
            columns.append(jnp.concatenate(blocks, axis=0).astype(BF16))
        return dot_tn(jnp.concatenate(columns, axis=1), make).reshape(count, 128, 256)

    def taps_of(ref, lead, first, count):
        parts = []
        for shift in range(3):
            for pair in range(2):
                part = ref[(*lead, pl.ds(first + pair, count), pl.ds(16 * shift, 128))]
                parts.append(part.reshape(count * 128, part.shape[-1]))
        return parts

    def within(layer):
        rows = []
        for shift in range(3):
            for pair in range(2):
                for r in (1, 0):
                    for y in range(2):
                        rows.append(
                            jnp.concatenate(
                                [unique[layer, r + 1 - to, 2 * pair + y, shift] for to in (1, 0)], axis=1
                            )
                        )
        return jnp.concatenate(rows, axis=0)

    def across(layer):
        rows = []
        none = jnp.zeros((64, 128), BF16)
        for shift in range(3):
            for pair in range(2):
                for y in range(2):
                    rows.append(jnp.concatenate([none, unique[layer, 0, 2 * pair + y, shift]], axis=1))
                for y in range(2):
                    rows.append(jnp.concatenate([unique[layer, 2, 2 * pair + y, shift], none], axis=1))
        return jnp.concatenate(rows, axis=0)

    def finish(total, layer, count, first_row, there):
        row = first_row + 2 * iota((count, 1, 256), 0) + ((iota((count, 1, 256), 2) >> 6) & 1)
        inside = (row >= 0) & (row < grid_rows) & there
        value = jnp.maximum(total + bias[layer], 0.0).reshape(count, 128, 256)
        return value * jnp.where(inside, 1.0, 0.0)

    def late_cells(j, b):
        tile = win[1, 1 + j + (b & 1)].astype(F32)
        at = (b >> 1) * 4 + (1 - (b & 1)) * 2
        return tile[at : at + 1], tile[at + 1 : at + 2]

    windows = ((0, True), (1, later))

    def begin(w, there, first, count):
        def cells(j, b):
            tile = win[2 * w, j].astype(F32)
            return tile[2 * b : 2 * b + 1], tile[2 * b + 1 : 2 * b + 2]

        put(ha, (w,), start(cells, first, count, base - 6, there), first, count)

    def first_layer(w, there, first, count):
        total = dot(jnp.concatenate(taps_of(ha, (w,), first, count), axis=1), within(0))
        put(hb, (w,), finish(total, 0, count, base - 5 + 2 * first, there), first, count)

    def middle_layer(w, there, first, count):
        total = dot(jnp.concatenate(taps_of(hb, (w,), first, count), axis=1), within(1))
        put(hc, (w,), finish(total, 1, count, base - 4 + 2 * first, there), first, count)

    def last_layer(w, there, first, count):
        total = dot(jnp.concatenate(taps_of(hc, (w,), first, count), axis=1), within(2))
        value = finish(total, 2, count, base - 3 + 2 * first, there)
        put(final, (w,), value[:, :, 128 * w : 128 * w + 128], first, count)
        if w == 0:
            ahead[first : first + count] = value[:, :, 128:256].astype(BF16)

    def pair_again(w, first, count):
        one, two = final[w, first : first + count].astype(F32), final[w, first + 1 : first + 1 + count].astype(F32)
        swapped = jnp.where(iota((count, 160, 128), 2) < 64, two, one)
        paired[w, first : first + count] = pltpu.roll(swapped, 64, 2).astype(BF16)

    pl.when(later)(to_earlier.wait_recv)
    for w, there in windows:
        begin(w, there, 3, 4)

    @pl.when(down)
    def _():
        pl.semaphore_wait(ready, 1)
        to_below.start()

    pl.when(down & later)(on_below.start)
    pl.when(up)(to_below.wait_recv)
    pl.when(up & later)(on_below.wait_recv)
    for w, there in windows:
        begin(w, there, 0, 3)
    for layer, count in ((first_layer, 6), (middle_layer, 5), (last_layer, 4)):
        for w, there in windows:
            layer(w, there, 0, count)
    put(hd, (0,), start(late_cells, 0, 5, base - 3, True), 0, 5)
    for w in range(2):
        pair_again(w, 0, 3)
    pl.when(down)(to_above.wait_recv)
    pl.when(down & later)(to_corner.wait_recv)
    for w, there in windows:
        begin(w, there, 7, 3)
    for layer, first in ((first_layer, 6), (middle_layer, 5), (last_layer, 4)):
        for w, there in windows:
            layer(w, there, first, 3)
    put(hd, (0,), start(late_cells, 5, 2, base - 3, True), 5, 2)
    for w in range(2):
        pair_again(w, 3, 3)

    def beside(ref, first, count):
        left = taps_of(ref, (0,), first, count)
        right = taps_of(ref, (1,), first, count)
        return [v for pair in zip(left, right) for v in pair]

    def second(own, others, layer, count, first_other):
        lhs = jnp.concatenate(taps_of(own, (0,), 0, count) + beside(others, first_other, count), axis=1)
        return dot(lhs, jnp.concatenate([within(layer), across(layer)], axis=0))

    put(hb, (0,), finish(second(hd, final, 0, 6, 0), 0, 6, base - 2, True), 0, 6)
    put(hc, (0,), finish(second(hb, paired, 1, 5, 0), 1, 5, base - 1, True), 0, 5)
    last = finish(second(hc, final, 2, 4, 1), 2, 4, base, True).astype(BF16).reshape(512, 256)

    w_terms = three_terms(quad(rw[...]))
    n = iota((32, 256), 0)
    weight = jnp.where(n >> 3 == 0, w_terms[0].astype(F32), jnp.where(n >> 3 == 1, w_terms[1].astype(F32), w_terms[2].astype(F32)))
    weight = jnp.where((n < 24) & ((n & 7) == iota((32, 256), 1) >> 6), weight, 0.0).astype(BF16)
    first = jnp.concatenate([final[0, 1:6, 16:144, :].reshape(640, 128), ahead[1:6].reshape(640, 128)], axis=1)
    a_sum = dot_nt(weight, first)
    b_sum = dot_nt(weight, last)
    a_sum = a_sum[0:8] + a_sum[8:16] + a_sum[16:24]
    b_sum = b_sum[0:8] + b_sum[8:16] + b_sum[16:24]
    y = iota((8, 128), 0)
    rounds = []
    for total, shift in ((a_sum, 1), (b_sum, 0)):
        for r in range(2):
            tile = jnp.zeros((8, 128), F32)
            for i in range(8):
                pair, inner = (i + shift) // 2, (i + shift) % 2
                b = (1 - r) * 2 + inner
                row = jnp.broadcast_to(total[b : b + 1, 128 * pair : 128 * pair + 128], (8, 128))
                tile = jnp.where(y == i, row, tile)
            rounds.append(tile)
    logits = jnp.concatenate(rounds, axis=0)
    back = one_hot(iota((128, 128), 1) == (iota((128, 128), 0) & 15) * 8 + (iota((128, 128), 0) >> 4))
    parts = dot(jnp.concatenate(three_terms(logits), axis=0), back)
    logits = (parts[0:32] + parts[32:64] + parts[64:96]).reshape(4, 8, 128)
    result[0] = logits
    out_ref[...] = logits

    pl.when(down)(to_below.wait_send)
    pl.when(up)(to_above.wait_send)
    pl.when(earlier)(to_earlier.wait_send)
    pl.when(later & down)(on_below.wait_send)
    pl.when(up & earlier)(to_corner.wait_send)


def kernel(
    spaces, times, lead,
    ev_hbm, so_hbm, emb_hbm, gain_hbm, cw_hbm, cb_hbm, rw_hbm,
    out_ref,
    ev, so, emb, gain, cw, cb, rw,
    win, unique, ha, hb, hc, hd, ahead, final, paired, result,
    load_sem, send_sem, recv_sem, hello, ready,
):
    space, time, core = lax.axis_index("space"), lax.axis_index("tm"), lax.axis_index("chan")
    worker = core == lax.axis_size("chan") - 1
    grid_rows = 8 * spaces
    up, down = space > 0, space < spaces - 1
    later, earlier = time < times - 1, time > 0
    barrier = pltpu.get_barrier_semaphore()

    def remote(src, dst, sent, got, device):
        return pltpu.make_async_remote_copy(
            src_ref=src, dst_ref=dst, send_sem=send_sem.at[sent], recv_sem=recv_sem.at[got],
            device_id=device, device_id_type=MESH,
        )

    def serves(j):
        return space >= j if j == lead else (space >= j) & (space == spaces - 1)

    gives = [
        remote(result.at[j], result.at[0], 5 + lead + j, 5, {"space": space - j, "chan": core - 1}) for j in range(lead + 1)
    ]

    @pl.when(jnp.logical_not(worker))
    def _():
        pl.semaphore_wait(barrier, 1)
        for j in range(lead + 1):
            @pl.when(space + lead <= spaces - 1 if j == lead else space == spaces - 1 - j)
            def _():
                pl.semaphore_signal(
                    hello.at[j], inc=1, device_id={"space": space + j, "chan": core + 1}, device_id_type=MESH
                )
        gives[0].wait_recv()
        out_ref[...] = result[0]

    @pl.when(worker)
    def _():
        loads = [
            pltpu.make_async_copy(src, dst, load_sem.at[i])
            for i, (src, dst) in enumerate(
                ((ev_hbm, ev), (so_hbm, so), (cw_hbm, cw), (emb_hbm, emb), (gain_hbm, gain), (cb_hbm, cb), (rw_hbm, rw))
            )
        ]
        for load in loads:
            load.start()

        def greet(there, device):
            @pl.when(there)
            def _():
                pl.semaphore_signal(barrier, inc=1, device_id=device, device_id_type=MESH)

        greet(down, {"space": space + 1})
        greet(later, {"tm": time + 1})
        greet(earlier, {"tm": time - 1})
        greet(down & later, {"space": space + 1, "tm": time + 1})
        for j in range(lead + 1):
            greet(serves(j), {"space": space - j, "chan": core - 1})

        compute(
            spaces, space, time, up, down, later, earlier, barrier, ready, grid_rows, remote, loads,
            out_ref, ev, so, emb, gain, cw, cb, rw, win, unique, ha, hb, hc, hd, ahead, final, paired, result,
        )

        passes = [remote(result.at[j], result.at[j + 1], 5 + j, 6 + j, {"space": space + 1}) for j in range(lead)]
        for j in range(lead + 1):
            if j > 0:
                pl.when(space >= j)(passes[j - 1].wait_recv)
            if j < lead:
                pl.when(down & (space >= j))(passes[j].start)
        for j in range(lead + 1):
            @pl.when(serves(j))
            def _():
                pl.semaphore_wait(hello.at[j], 1)
                gives[j].start()
        for j in range(lead):
            pl.when(down & (space >= j))(passes[j].wait_send)
        for j in range(lead + 1):
            pl.when(serves(j))(gives[j].wait_send)


def per_device(spaces, times, events, soft_info, embed, soft_gain, conv_weights, conv_bias, readout_weight):
    layers, channels, taps = conv_weights.shape
    gain = soft_gain.reshape(1, channels)
    readout = readout_weight.reshape(1, channels)
    lead = min(LEAD, spaces - 1)
    any_space = pl.BlockSpec(memory_space=pl.ANY)
    return pl.pallas_call(
        functools.partial(kernel, spaces, times, lead),
        out_shape=jax.ShapeDtypeStruct(events.shape, F32),
        in_specs=[any_space] * 7,
        out_specs=pl.BlockSpec(memory_space=pltpu.VMEM),
        scratch_shapes=[
            pltpu.VMEM(events.shape, jnp.int32),
            pltpu.VMEM(soft_info.shape, BF16),
            pltpu.VMEM(embed.shape, F32),
            pltpu.VMEM(gain.shape, F32),
            pltpu.VMEM(conv_weights.shape, BF16),
            pltpu.VMEM(conv_bias.shape, F32),
            pltpu.VMEM(readout.shape, F32),
            pltpu.VMEM((3, 10, 8, 128), BF16),
            pltpu.VMEM((layers, 3, 4, 3, channels, 128), BF16),
            pltpu.VMEM((2, 10, 160, 256), BF16),
            pltpu.VMEM((2, 9, 160, 256), BF16),
            pltpu.VMEM((2, 8, 160, 256), BF16),
            pltpu.VMEM((1, 7, 160, 256), BF16),
            pltpu.VMEM((7, 128, 128), BF16),
            pltpu.VMEM((2, 7, 160, 128), BF16),
            pltpu.VMEM((2, 6, 160, 128), BF16),
            pltpu.VMEM((lead + 1, *events.shape), F32),
            pltpu.SemaphoreType.DMA((7,)),
            pltpu.SemaphoreType.DMA((6 + 2 * lead,)),
            pltpu.SemaphoreType.DMA((6 + lead,)),
            pltpu.SemaphoreType.REGULAR((lead + 1,)),
            pltpu.SemaphoreType.REGULAR,
        ],
        compiler_params=pltpu.CompilerParams(collective_id=0, has_side_effects=True, vmem_limit_bytes=48 * 1024 * 1024),
    )(*[pltpu.with_memory_space_constraint(v, pltpu.HBM) for v in (events, soft_info, embed, gain, conv_weights, conv_bias, readout)])


def solution(mesh):
    tiled = P(("parts", "tm"), "space", None)
    return jax.shard_map(
        functools.partial(per_device, mesh.shape["space"], mesh.shape["tm"]),
        mesh=mesh, in_specs=(tiled, tiled, P(), P(), P(), P(), P()), out_specs=tiled, check_vma=False,
    )
```

```python
import functools

import jax
import jax.numpy as jnp
from jax import lax
from jax.experimental import pallas as pl
from jax.experimental.pallas import tpu as pltpu
from jax.sharding import PartitionSpec as P

F32 = jnp.float32
BF16 = jnp.bfloat16
MESH = pl.DeviceIdType.MESH
LEAD = 5


def iota(shape, dim):
    return lax.broadcasted_iota(jnp.int32, shape, dim)


def three_terms(value):
    high = value.astype(BF16)
    rest = value - high.astype(F32)
    middle = rest.astype(BF16)
    low = (rest - middle.astype(F32)).astype(BF16)
    return high, middle, low


def one_hot(condition):
    return jnp.where(condition, 1.0, 0.0).astype(BF16)


def dot(a, b):
    return lax.dot_general(a, b, (((1,), (0,)), ((), ())), preferred_element_type=F32)


def dot_nt(a, b):
    return lax.dot_general(a, b, (((1,), (1,)), ((), ())), preferred_element_type=F32)


def dot_tn(a, b):
    return lax.dot_general(a, b, (((0,), (0,)), ((), ())), preferred_element_type=F32)


def quad(row):
    return jnp.concatenate([row] * 4, axis=1)


def put(ref, lead, value, first, count):
    width = value.shape[2]
    q = iota((count, 16, width), 1)
    last, head = value[:, 112:128], value[:, 0:16]
    before = jnp.where(q == 0, 0.0, pltpu.roll(last, 1, 1))
    after = jnp.where(q == 15, 0.0, pltpu.roll(head, 15, 1))
    ref[(*lead, pl.ds(first, count), pl.ds(0, 16))] = before.astype(BF16)
    ref[(*lead, pl.ds(first, count), pl.ds(16, 128))] = value.astype(BF16)
    ref[(*lead, pl.ds(first, count), pl.ds(144, 16))] = after.astype(BF16)


def compute(
    spaces, space, time, near, up, down, later, earlier, barrier, ready, grid_rows, remote, loads,
    out_ref, ev, so, emb, gain, cw, cb, rw, win, unique, ha, hb, hc, hd, ahead, final, paired, result,
):
    spread = one_hot(iota((128, 128), 0) == (iota((128, 128), 1) & 15) * 8 + (iota((128, 128), 1) >> 4))
    m = iota((64, 64), 0)
    source = (
        (m & 1) * 32 + ((m >> 5) * 2 + 1 - ((m >> 2) & 1)) * 8 + ((m >> 3) & 3) * 2 + ((m >> 1) & 1)
    )
    order = one_hot(iota((64, 64), 1) == source)
    loads[0].wait()
    loads[1].wait()
    raw = jnp.concatenate([ev[...].astype(F32).reshape(32, 128), so[...].astype(F32).reshape(32, 128)], axis=0)
    staged = dot(order, dot(raw.astype(BF16), spread).astype(BF16)).reshape(2, 4, 8, 128).astype(BF16)
    win[0, 3:7] = staged[0]
    win[1, 3:7] = staged[1]

    to_below = remote(win.at[0:2, 4:7], win.at[0:2, 0:3], 0, 0, {"space": space + 1})
    to_above = remote(win.at[0:2, 3:6], win.at[0:2, 7:10], 1, 1, {"space": space - 1})
    to_earlier = remote(win.at[0, 3:7], win.at[2, 3:7], 2, 2, {"tm": time - 1})
    on_below = remote(win.at[2, 4:7], win.at[2, 0:3], 3, 3, {"space": space + 1})
    to_corner = remote(win.at[0, 3:6], win.at[2, 7:10], 4, 4, {"space": space - 1, "tm": time - 1})

    pl.semaphore_wait(
        barrier,
        jnp.where(up, 1, 0) + jnp.where(later, 1, 0) + jnp.where(earlier, 1, 0) + jnp.where(up & earlier, 1, 0)
        + jnp.where(near, 1, 0),
    )
    pl.when(up)(to_above.start)
    pl.when(up & earlier)(to_corner.start)
    pl.when(earlier)(to_earlier.start)

    @pl.when(up)
    def _():
        pl.semaphore_signal(ready, inc=1, device_id={"space": space - 1}, device_id_type=MESH)

    loads[2].wait()
    blank = jnp.zeros((3, 1, 3, 16, 128), F32)
    for half in range(4):
        pieces = []
        for chunk in (2 * half, 2 * half + 1):
            begin = 216 * chunk // 128 * 128
            stop = min(-(-(216 * chunk + 216) // 128) * 128, cw.shape[2])
            n = iota((216, stop - begin), 0)
            select = one_hot(iota((216, stop - begin), 1) == (n & 7) * 27 + (n >> 3) + (216 * chunk - begin))
            taps = [cw[layer, :, begin:stop] for layer in range(3)]
            two = dot_nt(select, jnp.concatenate([taps[0], taps[0], taps[1], taps[1]], axis=0))
            one = dot_nt(select, jnp.concatenate([taps[2], taps[2]], axis=0))
            pieces.append([v.reshape(27, 8, 128) for v in (two[:, :128], two[:, 128:], one)])
        for layer in range(3):
            tap = jnp.concatenate([pieces[0][layer], pieces[1][layer]], axis=1).reshape(3, 3, 3, 16, 128)
            low = jnp.concatenate([tap, blank], axis=1)
            high = jnp.concatenate([blank, tap], axis=1)
            both = jnp.where(iota((3, 4, 3, 16, 128), 4) < 64, low, high)
            unique[layer, :, :, :, 16 * half : 16 * half + 16, :] = both.astype(BF16)

    for load in loads[3:]:
        load.wait()
    e_terms = three_terms(quad(emb[...]))
    g_terms = three_terms(quad(gain[...]))
    column = jnp.concatenate(
        [t.astype(F32) for t in e_terms] + [t.astype(F32) for t in g_terms] + [jnp.zeros((1, 256), F32)], axis=0
    )
    make = jnp.where(
        iota((64, 256), 0) >> 4 == iota((64, 256), 1) >> 6, jnp.concatenate([column] * 4, axis=0), 0.0
    ).astype(BF16)
    bias = [quad(cb[layer : layer + 1, :]) for layer in range(3)]

    base = 8 * space
    k = iota((16, 128), 0)
    column_parity = iota((16, 128), 1) >> 4

    def inputs(cell, row, there):
        event, signal = cell
        inside = (row >= 0) & (row < grid_rows) & there
        code = 2 * ((column_parity + row) & 1) + event.astype(jnp.int32)
        value = jnp.where(k < 12, jnp.where(code == (k & 3), 1.0, 0.0), jnp.where(k < 15, signal, 0.0))
        return jnp.where(inside, value, 0.0)

    def start(cells, first, count, first_row, there):
        columns = []
        for j in range(first, first + count):
            blocks = []
            for b in range(4):
                blocks.append(inputs(cells(j, b), first_row + 2 * j + (b & 1), there))
            columns.append(jnp.concatenate(blocks, axis=0).astype(BF16))
        return dot_tn(jnp.concatenate(columns, axis=1), make).reshape(count, 128, 256)

    def taps_of(ref, lead, first, count):
        parts = []
        for shift in range(3):
            for pair in range(2):
                part = ref[(*lead, pl.ds(first + pair, count), pl.ds(16 * shift, 128))]
                parts.append(part.reshape(count * 128, part.shape[-1]))
        return parts

    def within(layer):
        rows = []
        for shift in range(3):
            for pair in range(2):
                for r in (1, 0):
                    for y in range(2):
                        rows.append(
                            jnp.concatenate(
                                [unique[layer, r + 1 - to, 2 * pair + y, shift] for to in (1, 0)], axis=1
                            )
                        )
        return jnp.concatenate(rows, axis=0)

    def across(layer):
        rows = []
        none = jnp.zeros((64, 128), BF16)
        for shift in range(3):
            for pair in range(2):
                for y in range(2):
                    rows.append(jnp.concatenate([none, unique[layer, 0, 2 * pair + y, shift]], axis=1))
                for y in range(2):
                    rows.append(jnp.concatenate([unique[layer, 2, 2 * pair + y, shift], none], axis=1))
        return jnp.concatenate(rows, axis=0)

    def finish(total, layer, count, first_row, there):
        row = first_row + 2 * iota((count, 1, 256), 0) + ((iota((count, 1, 256), 2) >> 6) & 1)
        inside = (row >= 0) & (row < grid_rows) & there
        value = jnp.maximum(total + bias[layer], 0.0).reshape(count, 128, 256)
        return value * jnp.where(inside, 1.0, 0.0)

    def late_cells(j, b):
        tile = win[1, 1 + j + (b & 1)].astype(F32)
        at = (b >> 1) * 4 + (1 - (b & 1)) * 2
        return tile[at : at + 1], tile[at + 1 : at + 2]

    windows = ((0, True), (1, later))

    def begin(w, there, first, count):
        def cells(j, b):
            tile = win[2 * w, j].astype(F32)
            return tile[2 * b : 2 * b + 1], tile[2 * b + 1 : 2 * b + 2]

        put(ha, (w,), start(cells, first, count, base - 6, there), first, count)

    def first_layer(w, there, first, count):
        total = dot(jnp.concatenate(taps_of(ha, (w,), first, count), axis=1), within(0))
        put(hb, (w,), finish(total, 0, count, base - 5 + 2 * first, there), first, count)

    def middle_layer(w, there, first, count):
        total = dot(jnp.concatenate(taps_of(hb, (w,), first, count), axis=1), within(1))
        put(hc, (w,), finish(total, 1, count, base - 4 + 2 * first, there), first, count)

    def last_layer(w, there, first, count):
        total = dot(jnp.concatenate(taps_of(hc, (w,), first, count), axis=1), within(2))
        value = finish(total, 2, count, base - 3 + 2 * first, there)
        put(final, (w,), value[:, :, 128 * w : 128 * w + 128], first, count)
        if w == 0:
            ahead[first : first + count] = value[:, :, 128:256].astype(BF16)

    def pair_again(w, first, count):
        one, two = final[w, first : first + count].astype(F32), final[w, first + 1 : first + 1 + count].astype(F32)
        swapped = jnp.where(iota((count, 160, 128), 2) < 64, two, one)
        paired[w, first : first + count] = pltpu.roll(swapped, 64, 2).astype(BF16)

    pl.when(later)(to_earlier.wait_recv)
    for w, there in windows:
        begin(w, there, 3, 4)

    @pl.when(down)
    def _():
        pl.semaphore_wait(ready, 1)
        to_below.start()

    pl.when(down & later)(on_below.start)
    pl.when(up)(to_below.wait_recv)
    pl.when(up & later)(on_below.wait_recv)
    for w, there in windows:
        begin(w, there, 0, 3)
    for layer, count in ((first_layer, 6), (middle_layer, 5), (last_layer, 4)):
        for w, there in windows:
            layer(w, there, 0, count)
    put(hd, (0,), start(late_cells, 0, 5, base - 3, True), 0, 5)
    for w in range(2):
        pair_again(w, 0, 3)
    pl.when(down)(to_above.wait_recv)
    pl.when(down & later)(to_corner.wait_recv)
    for w, there in windows:
        begin(w, there, 7, 3)
    for layer, first in ((first_layer, 6), (middle_layer, 5), (last_layer, 4)):
        for w, there in windows:
            layer(w, there, first, 3)
    put(hd, (0,), start(late_cells, 5, 2, base - 3, True), 5, 2)
    for w in range(2):
        pair_again(w, 3, 3)

    def beside(ref, first, count):
        left = taps_of(ref, (0,), first, count)
        right = taps_of(ref, (1,), first, count)
        return [v for pair in zip(left, right) for v in pair]

    def second(own, others, layer, count, first_other):
        lhs = jnp.concatenate(taps_of(own, (0,), 0, count) + beside(others, first_other, count), axis=1)
        return dot(lhs, jnp.concatenate([within(layer), across(layer)], axis=0))

    put(hb, (0,), finish(second(hd, final, 0, 6, 0), 0, 6, base - 2, True), 0, 6)
    put(hc, (0,), finish(second(hb, paired, 1, 5, 0), 1, 5, base - 1, True), 0, 5)
    last = finish(second(hc, final, 2, 4, 1), 2, 4, base, True).astype(BF16).reshape(512, 256)

    w_terms = three_terms(quad(rw[...]))
    n = iota((32, 256), 0)
    weight = jnp.where(n >> 3 == 0, w_terms[0].astype(F32), jnp.where(n >> 3 == 1, w_terms[1].astype(F32), w_terms[2].astype(F32)))
    weight = jnp.where((n < 24) & ((n & 7) == iota((32, 256), 1) >> 6), weight, 0.0).astype(BF16)
    first = jnp.concatenate([final[0, 1:6, 16:144, :].reshape(640, 128), ahead[1:6].reshape(640, 128)], axis=1)
    a_sum = dot_nt(weight, first)
    b_sum = dot_nt(weight, last)
    a_sum = a_sum[0:8] + a_sum[8:16] + a_sum[16:24]
    b_sum = b_sum[0:8] + b_sum[8:16] + b_sum[16:24]
    y = iota((8, 128), 0)
    rounds = []
    for total, shift in ((a_sum, 1), (b_sum, 0)):
        for r in range(2):
            tile = jnp.zeros((8, 128), F32)
            for i in range(8):
                pair, inner = (i + shift) // 2, (i + shift) % 2
                b = (1 - r) * 2 + inner
                row = jnp.broadcast_to(total[b : b + 1, 128 * pair : 128 * pair + 128], (8, 128))
                tile = jnp.where(y == i, row, tile)
            rounds.append(tile)
    logits = jnp.concatenate(rounds, axis=0)
    back = one_hot(iota((128, 128), 1) == (iota((128, 128), 0) & 15) * 8 + (iota((128, 128), 0) >> 4))
    parts = dot(jnp.concatenate(three_terms(logits), axis=0), back)
    logits = (parts[0:32] + parts[32:64] + parts[64:96]).reshape(4, 8, 128)
    result[0] = logits
    out_ref[...] = logits

    pl.when(down)(to_below.wait_send)
    pl.when(up)(to_above.wait_send)
    pl.when(earlier)(to_earlier.wait_send)
    pl.when(later & down)(on_below.wait_send)
    pl.when(up & earlier)(to_corner.wait_send)


def kernel(
    spaces, times, lead,
    ev_hbm, so_hbm, emb_hbm, gain_hbm, cw_hbm, cb_hbm, rw_hbm,
    out_ref,
    ev, so, emb, gain, cw, cb, rw,
    win, unique, ha, hb, hc, hd, ahead, final, paired, result,
    load_sem, send_sem, recv_sem, hello, taker, ready,
):
    space, time, core = lax.axis_index("space"), lax.axis_index("tm"), lax.axis_index("chan")
    worker = core == lax.axis_size("chan") - 1
    grid_rows = 8 * spaces
    up, down = space > 0, space < spaces - 1
    later, earlier = time < times - 1, time > 0
    barrier = pltpu.get_barrier_semaphore()

    def remote(src, dst, sent, got, device):
        return pltpu.make_async_remote_copy(
            src_ref=src, dst_ref=dst, send_sem=send_sem.at[sent], recv_sem=recv_sem.at[got],
            device_id=device, device_id_type=MESH,
        )

    first = space == 0 if lead > 0 else space < 0
    keeper = space == lead if lead > 0 else space < 0
    near = jnp.logical_not(first)
    give = remote(result.at[0], result.at[0], 5, 5, {"chan": core - 1})
    keep = remote(result.at[0], result.at[1], 6, 6, {"space": space + lead, "chan": core - 1})
    serve = remote(result.at[1], result.at[0], 7, 5, {"space": space - lead})

    def signal(there, semaphore, device):
        @pl.when(there)
        def _():
            pl.semaphore_signal(semaphore, inc=1, device_id=device, device_id_type=MESH)

    @pl.when(jnp.logical_not(worker))
    def _():
        signal(near, barrier, {"chan": core + 1})
        signal(keeper, barrier, {"space": space - lead})

        @pl.when(first | keeper)
        def _():
            pl.semaphore_wait(barrier, 1)

        signal(first, hello, {"space": space + lead})
        signal(keeper, taker, {"space": space - lead, "chan": core + 1})

        @pl.when(keeper)
        def _():
            keep.wait_recv()
            pl.semaphore_wait(hello, 1)
            serve.start()

        give.wait_recv()
        out_ref[...] = result[0]
        pl.when(keeper)(serve.wait_send)

    @pl.when(worker)
    def _():
        loads = [
            pltpu.make_async_copy(src, dst, load_sem.at[i])
            for i, (src, dst) in enumerate(
                ((ev_hbm, ev), (so_hbm, so), (cw_hbm, cw), (emb_hbm, emb), (gain_hbm, gain), (cb_hbm, cb), (rw_hbm, rw))
            )
        ]
        for load in loads:
            load.start()

        signal(first, barrier, {"space": space + lead, "chan": core - 1})
        signal(down, barrier, {"space": space + 1})
        signal(later, barrier, {"tm": time + 1})
        signal(earlier, barrier, {"tm": time - 1})
        signal(down & later, barrier, {"space": space + 1, "tm": time + 1})
        compute(
            spaces, space, time, near, up, down, later, earlier, barrier, ready, grid_rows, remote, loads,
            out_ref, ev, so, emb, gain, cw, cb, rw, win, unique, ha, hb, hc, hd, ahead, final, paired, result,
        )

        pl.when(near)(give.start)

        @pl.when(first)
        def _():
            pl.semaphore_wait(taker, 1)
            keep.start()

        pl.when(near)(give.wait_send)
        pl.when(first)(keep.wait_send)


def per_device(spaces, times, events, soft_info, embed, soft_gain, conv_weights, conv_bias, readout_weight):
    layers, channels, taps = conv_weights.shape
    gain = soft_gain.reshape(1, channels)
    readout = readout_weight.reshape(1, channels)
    lead = min(LEAD, spaces - 1)
    any_space = pl.BlockSpec(memory_space=pl.ANY)
    return pl.pallas_call(
        functools.partial(kernel, spaces, times, lead),
        out_shape=jax.ShapeDtypeStruct(events.shape, F32),
        in_specs=[any_space] * 7,
        out_specs=pl.BlockSpec(memory_space=pltpu.VMEM),
        scratch_shapes=[
            pltpu.VMEM(events.shape, jnp.int32),
            pltpu.VMEM(soft_info.shape, BF16),
            pltpu.VMEM(embed.shape, F32),
            pltpu.VMEM(gain.shape, F32),
            pltpu.VMEM(conv_weights.shape, BF16),
            pltpu.VMEM(conv_bias.shape, F32),
            pltpu.VMEM(readout.shape, F32),
            pltpu.VMEM((3, 10, 8, 128), BF16),
            pltpu.VMEM((layers, 3, 4, 3, channels, 128), BF16),
            pltpu.VMEM((2, 10, 160, 256), BF16),
            pltpu.VMEM((2, 9, 160, 256), BF16),
            pltpu.VMEM((2, 8, 160, 256), BF16),
            pltpu.VMEM((1, 7, 160, 256), BF16),
            pltpu.VMEM((7, 128, 128), BF16),
            pltpu.VMEM((2, 7, 160, 128), BF16),
            pltpu.VMEM((2, 6, 160, 128), BF16),
            pltpu.VMEM((2, *events.shape), F32),
            pltpu.SemaphoreType.DMA((7,)),
            pltpu.SemaphoreType.DMA((8,)),
            pltpu.SemaphoreType.DMA((7,)),
            pltpu.SemaphoreType.REGULAR,
            pltpu.SemaphoreType.REGULAR,
            pltpu.SemaphoreType.REGULAR,
        ],
        compiler_params=pltpu.CompilerParams(collective_id=0, has_side_effects=True, vmem_limit_bytes=48 * 1024 * 1024),
    )(*[pltpu.with_memory_space_constraint(v, pltpu.HBM) for v in (events, soft_info, embed, gain, conv_weights, conv_bias, readout)])


def solution(mesh):
    tiled = P(("parts", "tm"), "space", None)
    return jax.shard_map(
        functools.partial(per_device, mesh.shape["space"], mesh.shape["tm"]),
        mesh=mesh, in_specs=(tiled, tiled, P(), P(), P(), P(), P()), out_specs=tiled, check_vma=False,
    )
```

```python
import functools

import jax
import jax.numpy as jnp
from jax import lax
from jax.experimental import pallas as pl
from jax.experimental.pallas import tpu as pltpu
from jax.sharding import PartitionSpec as P

F32 = jnp.float32
BF16 = jnp.bfloat16
MESH = pl.DeviceIdType.MESH
LEAD = 4, 6


def iota(shape, dim):
    return lax.broadcasted_iota(jnp.int32, shape, dim)


def three_terms(value):
    high = value.astype(BF16)
    rest = value - high.astype(F32)
    middle = rest.astype(BF16)
    low = (rest - middle.astype(F32)).astype(BF16)
    return high, middle, low


def one_hot(condition):
    return jnp.where(condition, 1.0, 0.0).astype(BF16)


def dot(a, b):
    return lax.dot_general(a, b, (((1,), (0,)), ((), ())), preferred_element_type=F32)


def dot_nt(a, b):
    return lax.dot_general(a, b, (((1,), (1,)), ((), ())), preferred_element_type=F32)


def dot_tn(a, b):
    return lax.dot_general(a, b, (((0,), (0,)), ((), ())), preferred_element_type=F32)


def quad(row):
    return jnp.concatenate([row] * 4, axis=1)


def put(ref, lead, value, first, count):
    width = value.shape[2]
    q = iota((count, 16, width), 1)
    last, head = value[:, 112:128], value[:, 0:16]
    before = jnp.where(q == 0, 0.0, pltpu.roll(last, 1, 1))
    after = jnp.where(q == 15, 0.0, pltpu.roll(head, 15, 1))
    ref[(*lead, pl.ds(first, count), pl.ds(0, 16))] = before.astype(BF16)
    ref[(*lead, pl.ds(first, count), pl.ds(16, 128))] = value.astype(BF16)
    ref[(*lead, pl.ds(first, count), pl.ds(144, 16))] = after.astype(BF16)


def compute(
    spaces, space, time, near, up, down, later, earlier, barrier, ready, grid_rows, remote, loads,
    out_ref, ev, so, emb, gain, cw, cb, rw, win, unique, ha, hb, hc, hd, ahead, final, paired, result,
):
    spread = one_hot(iota((128, 128), 0) == (iota((128, 128), 1) & 15) * 8 + (iota((128, 128), 1) >> 4))
    m = iota((64, 64), 0)
    source = (
        (m & 1) * 32 + ((m >> 5) * 2 + 1 - ((m >> 2) & 1)) * 8 + ((m >> 3) & 3) * 2 + ((m >> 1) & 1)
    )
    order = one_hot(iota((64, 64), 1) == source)
    loads[0].wait()
    loads[1].wait()
    raw = jnp.concatenate([ev[...].astype(F32).reshape(32, 128), so[...].astype(F32).reshape(32, 128)], axis=0)
    staged = dot(order, dot(raw.astype(BF16), spread).astype(BF16)).reshape(2, 4, 8, 128).astype(BF16)
    win[0, 3:7] = staged[0]
    win[1, 3:7] = staged[1]

    to_below = remote(win.at[0:2, 4:7], win.at[0:2, 0:3], 0, 0, {"space": space + 1})
    to_above = remote(win.at[0:2, 3:6], win.at[0:2, 7:10], 1, 1, {"space": space - 1})
    to_earlier = remote(win.at[0, 3:7], win.at[2, 3:7], 2, 2, {"tm": time - 1})
    on_below = remote(win.at[2, 4:7], win.at[2, 0:3], 3, 3, {"space": space + 1})
    to_corner = remote(win.at[0, 3:6], win.at[2, 7:10], 4, 4, {"space": space - 1, "tm": time - 1})

    pl.semaphore_wait(
        barrier,
        jnp.where(up, 1, 0) + jnp.where(later, 1, 0) + jnp.where(earlier, 1, 0) + jnp.where(up & earlier, 1, 0)
        + jnp.where(near, 1, 0),
    )
    pl.when(up)(to_above.start)
    pl.when(up & earlier)(to_corner.start)
    pl.when(earlier)(to_earlier.start)

    @pl.when(up)
    def _():
        pl.semaphore_signal(ready, inc=1, device_id={"space": space - 1}, device_id_type=MESH)

    loads[2].wait()
    blank = jnp.zeros((3, 1, 3, 16, 128), F32)
    for half in range(4):
        pieces = []
        for chunk in (2 * half, 2 * half + 1):
            begin = 216 * chunk // 128 * 128
            stop = min(-(-(216 * chunk + 216) // 128) * 128, cw.shape[2])
            n = iota((216, stop - begin), 0)
            select = one_hot(iota((216, stop - begin), 1) == (n & 7) * 27 + (n >> 3) + (216 * chunk - begin))
            taps = [cw[layer, :, begin:stop] for layer in range(3)]
            two = dot_nt(select, jnp.concatenate([taps[0], taps[0], taps[1], taps[1]], axis=0))
            one = dot_nt(select, jnp.concatenate([taps[2], taps[2]], axis=0))
            pieces.append([v.reshape(27, 8, 128) for v in (two[:, :128], two[:, 128:], one)])
        for layer in range(3):
            tap = jnp.concatenate([pieces[0][layer], pieces[1][layer]], axis=1).reshape(3, 3, 3, 16, 128)
            low = jnp.concatenate([tap, blank], axis=1)
            high = jnp.concatenate([blank, tap], axis=1)
            both = jnp.where(iota((3, 4, 3, 16, 128), 4) < 64, low, high)
            unique[layer, :, :, :, 16 * half : 16 * half + 16, :] = both.astype(BF16)

    for load in loads[3:]:
        load.wait()
    e_terms = three_terms(quad(emb[...]))
    g_terms = three_terms(quad(gain[...]))
    column = jnp.concatenate(
        [t.astype(F32) for t in e_terms] + [t.astype(F32) for t in g_terms] + [jnp.zeros((1, 256), F32)], axis=0
    )
    make = jnp.where(
        iota((64, 256), 0) >> 4 == iota((64, 256), 1) >> 6, jnp.concatenate([column] * 4, axis=0), 0.0
    ).astype(BF16)
    bias = [quad(cb[layer : layer + 1, :]) for layer in range(3)]

    base = 8 * space
    k = iota((16, 128), 0)
    column_parity = iota((16, 128), 1) >> 4

    def inputs(cell, row, there):
        event, signal = cell
        inside = (row >= 0) & (row < grid_rows) & there
        code = 2 * ((column_parity + row) & 1) + event.astype(jnp.int32)
        value = jnp.where(k < 12, jnp.where(code == (k & 3), 1.0, 0.0), jnp.where(k < 15, signal, 0.0))
        return jnp.where(inside, value, 0.0)

    def start(cells, first, count, first_row, there):
        columns = []
        for j in range(first, first + count):
            blocks = []
            for b in range(4):
                blocks.append(inputs(cells(j, b), first_row + 2 * j + (b & 1), there))
            columns.append(jnp.concatenate(blocks, axis=0).astype(BF16))
        return dot_tn(jnp.concatenate(columns, axis=1), make).reshape(count, 128, 256)

    def taps_of(ref, lead, first, count):
        parts = []
        for shift in range(3):
            for pair in range(2):
                part = ref[(*lead, pl.ds(first + pair, count), pl.ds(16 * shift, 128))]
                parts.append(part.reshape(count * 128, part.shape[-1]))
        return parts

    def within(layer):
        rows = []
        for shift in range(3):
            for pair in range(2):
                for r in (1, 0):
                    for y in range(2):
                        rows.append(
                            jnp.concatenate(
                                [unique[layer, r + 1 - to, 2 * pair + y, shift] for to in (1, 0)], axis=1
                            )
                        )
        return jnp.concatenate(rows, axis=0)

    def across(layer):
        rows = []
        none = jnp.zeros((64, 128), BF16)
        for shift in range(3):
            for pair in range(2):
                for y in range(2):
                    rows.append(jnp.concatenate([none, unique[layer, 0, 2 * pair + y, shift]], axis=1))
                for y in range(2):
                    rows.append(jnp.concatenate([unique[layer, 2, 2 * pair + y, shift], none], axis=1))
        return jnp.concatenate(rows, axis=0)

    def finish(total, layer, count, first_row, there):
        row = first_row + 2 * iota((count, 1, 256), 0) + ((iota((count, 1, 256), 2) >> 6) & 1)
        inside = (row >= 0) & (row < grid_rows) & there
        value = jnp.maximum(total + bias[layer], 0.0).reshape(count, 128, 256)
        return value * jnp.where(inside, 1.0, 0.0)

    def late_cells(j, b):
        tile = win[1, 1 + j + (b & 1)].astype(F32)
        at = (b >> 1) * 4 + (1 - (b & 1)) * 2
        return tile[at : at + 1], tile[at + 1 : at + 2]

    windows = ((0, True), (1, later))

    def begin(w, there, first, count):
        def cells(j, b):
            tile = win[2 * w, j].astype(F32)
            return tile[2 * b : 2 * b + 1], tile[2 * b + 1 : 2 * b + 2]

        put(ha, (w,), start(cells, first, count, base - 6, there), first, count)

    def first_layer(w, there, first, count):
        total = dot(jnp.concatenate(taps_of(ha, (w,), first, count), axis=1), within(0))
        put(hb, (w,), finish(total, 0, count, base - 5 + 2 * first, there), first, count)

    def middle_layer(w, there, first, count):
        total = dot(jnp.concatenate(taps_of(hb, (w,), first, count), axis=1), within(1))
        put(hc, (w,), finish(total, 1, count, base - 4 + 2 * first, there), first, count)

    def last_layer(w, there, first, count):
        total = dot(jnp.concatenate(taps_of(hc, (w,), first, count), axis=1), within(2))
        value = finish(total, 2, count, base - 3 + 2 * first, there)
        put(final, (w,), value[:, :, 128 * w : 128 * w + 128], first, count)
        if w == 0:
            ahead[first : first + count] = value[:, :, 128:256].astype(BF16)

    def pair_again(w, first, count):
        one, two = final[w, first : first + count].astype(F32), final[w, first + 1 : first + 1 + count].astype(F32)
        swapped = jnp.where(iota((count, 160, 128), 2) < 64, two, one)
        paired[w, first : first + count] = pltpu.roll(swapped, 64, 2).astype(BF16)

    pl.when(later)(to_earlier.wait_recv)
    for w, there in windows:
        begin(w, there, 3, 4)

    @pl.when(down)
    def _():
        pl.semaphore_wait(ready, 1)
        to_below.start()

    pl.when(down & later)(on_below.start)
    pl.when(up)(to_below.wait_recv)
    pl.when(up & later)(on_below.wait_recv)
    for w, there in windows:
        begin(w, there, 0, 3)
    for layer, count in ((first_layer, 6), (middle_layer, 5), (last_layer, 4)):
        for w, there in windows:
            layer(w, there, 0, count)
    put(hd, (0,), start(late_cells, 0, 5, base - 3, True), 0, 5)
    for w in range(2):
        pair_again(w, 0, 3)
    pl.when(down)(to_above.wait_recv)
    pl.when(down & later)(to_corner.wait_recv)
    for w, there in windows:
        begin(w, there, 7, 3)
    for layer, first in ((first_layer, 6), (middle_layer, 5), (last_layer, 4)):
        for w, there in windows:
            layer(w, there, first, 3)
    put(hd, (0,), start(late_cells, 5, 2, base - 3, True), 5, 2)
    for w in range(2):
        pair_again(w, 3, 3)

    def beside(ref, first, count):
        left = taps_of(ref, (0,), first, count)
        right = taps_of(ref, (1,), first, count)
        return [v for pair in zip(left, right) for v in pair]

    def second(own, others, layer, count, first_other):
        lhs = jnp.concatenate(taps_of(own, (0,), 0, count) + beside(others, first_other, count), axis=1)
        return dot(lhs, jnp.concatenate([within(layer), across(layer)], axis=0))

    put(hb, (0,), finish(second(hd, final, 0, 6, 0), 0, 6, base - 2, True), 0, 6)
    put(hc, (0,), finish(second(hb, paired, 1, 5, 0), 1, 5, base - 1, True), 0, 5)
    last = finish(second(hc, final, 2, 4, 1), 2, 4, base, True).astype(BF16).reshape(512, 256)

    w_terms = three_terms(quad(rw[...]))
    n = iota((32, 256), 0)
    weight = jnp.where(n >> 3 == 0, w_terms[0].astype(F32), jnp.where(n >> 3 == 1, w_terms[1].astype(F32), w_terms[2].astype(F32)))
    weight = jnp.where((n < 24) & ((n & 7) == iota((32, 256), 1) >> 6), weight, 0.0).astype(BF16)
    first = jnp.concatenate([final[0, 1:6, 16:144, :].reshape(640, 128), ahead[1:6].reshape(640, 128)], axis=1)
    a_sum = dot_nt(weight, first)
    b_sum = dot_nt(weight, last)
    a_sum = a_sum[0:8] + a_sum[8:16] + a_sum[16:24]
    b_sum = b_sum[0:8] + b_sum[8:16] + b_sum[16:24]
    y = iota((8, 128), 0)
    rounds = []
    for total, shift in ((a_sum, 1), (b_sum, 0)):
        for r in range(2):
            tile = jnp.zeros((8, 128), F32)
            for i in range(8):
                pair, inner = (i + shift) // 2, (i + shift) % 2
                b = (1 - r) * 2 + inner
                row = jnp.broadcast_to(total[b : b + 1, 128 * pair : 128 * pair + 128], (8, 128))
                tile = jnp.where(y == i, row, tile)
            rounds.append(tile)
    logits = jnp.concatenate(rounds, axis=0)
    back = one_hot(iota((128, 128), 1) == (iota((128, 128), 0) & 15) * 8 + (iota((128, 128), 0) >> 4))
    parts = dot(jnp.concatenate(three_terms(logits), axis=0), back)
    logits = (parts[0:32] + parts[32:64] + parts[64:96]).reshape(4, 8, 128)
    result[0] = logits
    out_ref[...] = logits

    pl.when(down)(to_below.wait_send)
    pl.when(up)(to_above.wait_send)
    pl.when(earlier)(to_earlier.wait_send)
    pl.when(later & down)(on_below.wait_send)
    pl.when(up & earlier)(to_corner.wait_send)


def kernel(
    spaces, times, lead,
    ev_hbm, so_hbm, emb_hbm, gain_hbm, cw_hbm, cb_hbm, rw_hbm,
    out_ref,
    ev, so, emb, gain, cw, cb, rw,
    win, unique, ha, hb, hc, hd, ahead, final, paired, result,
    load_sem, send_sem, recv_sem, hello, taker, ready,
):
    space, time, core = lax.axis_index("space"), lax.axis_index("tm"), lax.axis_index("chan")
    worker = core == lax.axis_size("chan") - 1
    grid_rows = 8 * spaces
    up, down = space > 0, space < spaces - 1
    later, earlier = time < times - 1, time > 0
    barrier = pltpu.get_barrier_semaphore()

    def remote(src, dst, sent, got, device):
        return pltpu.make_async_remote_copy(
            src_ref=src, dst_ref=dst, send_sem=send_sem.at[sent], recv_sem=recv_sem.at[got],
            device_id=device, device_id_type=MESH,
        )

    halfway, whole = lead
    far = whole > 1
    first = space == 0 if far else space < 0
    relay = space == halfway if far else space < 0
    keeper = space == whole if far else space < 0
    near = jnp.logical_not(first)
    give = remote(result.at[0], result.at[0], 5, 5, {"chan": core - 1})
    keep = remote(result.at[0], result.at[1], 6, 6, {"space": space + halfway, "chan": core - 1})
    pass_on = remote(result.at[1], result.at[1], 7, 6, {"space": space + whole - halfway})
    serve = remote(result.at[1], result.at[0], 7, 5, {"space": space - whole})

    def signal(there, semaphore, device):
        @pl.when(there)
        def _():
            pl.semaphore_signal(semaphore, inc=1, device_id=device, device_id_type=MESH)

    @pl.when(jnp.logical_not(worker))
    def _():
        signal(near, barrier, {"chan": core + 1})
        signal(relay, barrier, {"space": space + whole - halfway})
        signal(keeper, barrier, {"space": space - whole})

        @pl.when(first | relay | keeper)
        def _():
            pl.semaphore_wait(barrier, 1)

        signal(first, hello, {"space": space + whole})
        signal(relay, taker, {"space": space - halfway, "chan": core + 1})
        signal(keeper, taker, {"space": space + halfway - whole})

        @pl.when(relay)
        def _():
            keep.wait_recv()
            pl.semaphore_wait(taker, 1)
            pass_on.start()

        @pl.when(keeper)
        def _():
            pass_on.wait_recv()
            pl.semaphore_wait(hello, 1)
            serve.start()

        give.wait_recv()
        out_ref[...] = result[0]
        pl.when(relay)(pass_on.wait_send)
        pl.when(keeper)(serve.wait_send)

    @pl.when(worker)
    def _():
        loads = [
            pltpu.make_async_copy(src, dst, load_sem.at[i])
            for i, (src, dst) in enumerate(
                ((ev_hbm, ev), (so_hbm, so), (cw_hbm, cw), (emb_hbm, emb), (gain_hbm, gain), (cb_hbm, cb), (rw_hbm, rw))
            )
        ]
        for load in loads:
            load.start()

        signal(first, barrier, {"space": space + halfway, "chan": core - 1})
        signal(down, barrier, {"space": space + 1})
        signal(later, barrier, {"tm": time + 1})
        signal(earlier, barrier, {"tm": time - 1})
        signal(down & later, barrier, {"space": space + 1, "tm": time + 1})
        compute(
            spaces, space, time, near, up, down, later, earlier, barrier, ready, grid_rows, remote, loads,
            out_ref, ev, so, emb, gain, cw, cb, rw, win, unique, ha, hb, hc, hd, ahead, final, paired, result,
        )

        pl.when(near)(give.start)

        @pl.when(first)
        def _():
            pl.semaphore_wait(taker, 1)
            keep.start()

        pl.when(near)(give.wait_send)
        pl.when(first)(keep.wait_send)


def per_device(spaces, times, events, soft_info, embed, soft_gain, conv_weights, conv_bias, readout_weight):
    layers, channels, taps = conv_weights.shape
    gain = soft_gain.reshape(1, channels)
    readout = readout_weight.reshape(1, channels)
    whole = min(LEAD[1], spaces - 1)
    lead = min(LEAD[0], whole - 1), whole
    any_space = pl.BlockSpec(memory_space=pl.ANY)
    return pl.pallas_call(
        functools.partial(kernel, spaces, times, lead),
        out_shape=jax.ShapeDtypeStruct(events.shape, F32),
        in_specs=[any_space] * 7,
        out_specs=pl.BlockSpec(memory_space=pltpu.VMEM),
        scratch_shapes=[
            pltpu.VMEM(events.shape, jnp.int32),
            pltpu.VMEM(soft_info.shape, BF16),
            pltpu.VMEM(embed.shape, F32),
            pltpu.VMEM(gain.shape, F32),
            pltpu.VMEM(conv_weights.shape, BF16),
            pltpu.VMEM(conv_bias.shape, F32),
            pltpu.VMEM(readout.shape, F32),
            pltpu.VMEM((3, 10, 8, 128), BF16),
            pltpu.VMEM((layers, 3, 4, 3, channels, 128), BF16),
            pltpu.VMEM((2, 10, 160, 256), BF16),
            pltpu.VMEM((2, 9, 160, 256), BF16),
            pltpu.VMEM((2, 8, 160, 256), BF16),
            pltpu.VMEM((1, 7, 160, 256), BF16),
            pltpu.VMEM((7, 128, 128), BF16),
            pltpu.VMEM((2, 7, 160, 128), BF16),
            pltpu.VMEM((2, 6, 160, 128), BF16),
            pltpu.VMEM((2, *events.shape), F32),
            pltpu.SemaphoreType.DMA((7,)),
            pltpu.SemaphoreType.DMA((8,)),
            pltpu.SemaphoreType.DMA((7,)),
            pltpu.SemaphoreType.REGULAR,
            pltpu.SemaphoreType.REGULAR,
            pltpu.SemaphoreType.REGULAR,
        ],
        compiler_params=pltpu.CompilerParams(collective_id=0, has_side_effects=True, vmem_limit_bytes=48 * 1024 * 1024),
    )(*[pltpu.with_memory_space_constraint(v, pltpu.HBM) for v in (events, soft_info, embed, gain, conv_weights, conv_bias, readout)])


def solution(mesh):
    tiled = P(("parts", "tm"), "space", None)
    return jax.shard_map(
        functools.partial(per_device, mesh.shape["space"], mesh.shape["tm"]),
        mesh=mesh, in_specs=(tiled, tiled, P(), P(), P(), P(), P()), out_specs=tiled, check_vma=False,
    )
```

```python
import functools

import jax
import jax.numpy as jnp
from jax import lax
from jax.experimental import pallas as pl
from jax.experimental.pallas import tpu as pltpu
from jax.sharding import PartitionSpec as P

F32 = jnp.float32
BF16 = jnp.bfloat16
MESH = pl.DeviceIdType.MESH
LEAD = 3, 5


def iota(shape, dim):
    return lax.broadcasted_iota(jnp.int32, shape, dim)


def three_terms(value):
    high = value.astype(BF16)
    rest = value - high.astype(F32)
    middle = rest.astype(BF16)
    low = (rest - middle.astype(F32)).astype(BF16)
    return high, middle, low


def one_hot(condition):
    return jnp.where(condition, 1.0, 0.0).astype(BF16)


def dot(a, b):
    return lax.dot_general(a, b, (((1,), (0,)), ((), ())), preferred_element_type=F32)


def dot_nt(a, b):
    return lax.dot_general(a, b, (((1,), (1,)), ((), ())), preferred_element_type=F32)


def dot_tn(a, b):
    return lax.dot_general(a, b, (((0,), (0,)), ((), ())), preferred_element_type=F32)


def quad(row):
    return jnp.concatenate([row] * 4, axis=1)


def put(ref, lead, value, first, count):
    width = value.shape[2]
    q = iota((count, 16, width), 1)
    last, head = value[:, 112:128], value[:, 0:16]
    before = jnp.where(q == 0, 0.0, pltpu.roll(last, 1, 1))
    after = jnp.where(q == 15, 0.0, pltpu.roll(head, 15, 1))
    ref[(*lead, pl.ds(first, count), pl.ds(0, 16))] = before.astype(BF16)
    ref[(*lead, pl.ds(first, count), pl.ds(16, 128))] = value.astype(BF16)
    ref[(*lead, pl.ds(first, count), pl.ds(144, 16))] = after.astype(BF16)


def compute(
    spaces, space, time, near, up, down, later, earlier, barrier, ready, grid_rows, remote, loads,
    out_ref, ev, so, emb, gain, cw, cb, rw, win, unique, ha, hb, hc, hd, ahead, final, paired, result,
):
    spread = one_hot(iota((128, 128), 0) == (iota((128, 128), 1) & 15) * 8 + (iota((128, 128), 1) >> 4))
    m = iota((64, 64), 0)
    source = (
        (m & 1) * 32 + ((m >> 5) * 2 + 1 - ((m >> 2) & 1)) * 8 + ((m >> 3) & 3) * 2 + ((m >> 1) & 1)
    )
    order = one_hot(iota((64, 64), 1) == source)
    loads[0].wait()
    loads[1].wait()
    raw = jnp.concatenate([ev[...].astype(F32).reshape(32, 128), so[...].astype(F32).reshape(32, 128)], axis=0)
    staged = dot(order, dot(raw.astype(BF16), spread).astype(BF16)).reshape(2, 4, 8, 128).astype(BF16)
    win[0, 3:7] = staged[0]
    win[1, 3:7] = staged[1]

    to_below = remote(win.at[0:2, 4:7], win.at[0:2, 0:3], 0, 0, {"space": space + 1})
    to_above = remote(win.at[0:2, 3:6], win.at[0:2, 7:10], 1, 1, {"space": space - 1})
    to_earlier = remote(win.at[0, 3:7], win.at[2, 3:7], 2, 2, {"tm": time - 1})
    on_below = remote(win.at[2, 4:7], win.at[2, 0:3], 3, 3, {"space": space + 1})
    to_corner = remote(win.at[0, 3:6], win.at[2, 7:10], 4, 4, {"space": space - 1, "tm": time - 1})

    pl.semaphore_wait(
        barrier,
        jnp.where(up, 1, 0) + jnp.where(later, 1, 0) + jnp.where(earlier, 1, 0) + jnp.where(up & earlier, 1, 0)
        + jnp.where(near, 1, 0),
    )
    pl.when(up)(to_above.start)
    pl.when(up & earlier)(to_corner.start)
    pl.when(earlier)(to_earlier.start)

    @pl.when(up)
    def _():
        pl.semaphore_signal(ready, inc=1, device_id={"space": space - 1}, device_id_type=MESH)

    loads[2].wait()
    blank = jnp.zeros((3, 1, 3, 16, 128), F32)
    for half in range(4):
        pieces = []
        for chunk in (2 * half, 2 * half + 1):
            begin = 216 * chunk // 128 * 128
            stop = min(-(-(216 * chunk + 216) // 128) * 128, cw.shape[2])
            n = iota((216, stop - begin), 0)
            select = one_hot(iota((216, stop - begin), 1) == (n & 7) * 27 + (n >> 3) + (216 * chunk - begin))
            taps = [cw[layer, :, begin:stop] for layer in range(3)]
            two = dot_nt(select, jnp.concatenate([taps[0], taps[0], taps[1], taps[1]], axis=0))
            one = dot_nt(select, jnp.concatenate([taps[2], taps[2]], axis=0))
            pieces.append([v.reshape(27, 8, 128) for v in (two[:, :128], two[:, 128:], one)])
        for layer in range(3):
            tap = jnp.concatenate([pieces[0][layer], pieces[1][layer]], axis=1).reshape(3, 3, 3, 16, 128)
            low = jnp.concatenate([tap, blank], axis=1)
            high = jnp.concatenate([blank, tap], axis=1)
            both = jnp.where(iota((3, 4, 3, 16, 128), 4) < 64, low, high)
            unique[layer, :, :, :, 16 * half : 16 * half + 16, :] = both.astype(BF16)

    for load in loads[3:]:
        load.wait()
    e_terms = three_terms(quad(emb[...]))
    g_terms = three_terms(quad(gain[...]))
    column = jnp.concatenate(
        [t.astype(F32) for t in e_terms] + [t.astype(F32) for t in g_terms] + [jnp.zeros((1, 256), F32)], axis=0
    )
    make = jnp.where(
        iota((64, 256), 0) >> 4 == iota((64, 256), 1) >> 6, jnp.concatenate([column] * 4, axis=0), 0.0
    ).astype(BF16)
    bias = [quad(cb[layer : layer + 1, :]) for layer in range(3)]

    base = 8 * space
    k = iota((16, 128), 0)
    column_parity = iota((16, 128), 1) >> 4

    def inputs(cell, row, there):
        event, signal = cell
        inside = (row >= 0) & (row < grid_rows) & there
        code = 2 * ((column_parity + row) & 1) + event.astype(jnp.int32)
        value = jnp.where(k < 12, jnp.where(code == (k & 3), 1.0, 0.0), jnp.where(k < 15, signal, 0.0))
        return jnp.where(inside, value, 0.0)

    def start(cells, first, count, first_row, there):
        columns = []
        for j in range(first, first + count):
            blocks = []
            for b in range(4):
                blocks.append(inputs(cells(j, b), first_row + 2 * j + (b & 1), there))
            columns.append(jnp.concatenate(blocks, axis=0).astype(BF16))
        return dot_tn(jnp.concatenate(columns, axis=1), make).reshape(count, 128, 256)

    def taps_of(ref, lead, first, count):
        parts = []
        for shift in range(3):
            for pair in range(2):
                part = ref[(*lead, pl.ds(first + pair, count), pl.ds(16 * shift, 128))]
                parts.append(part.reshape(count * 128, part.shape[-1]))
        return parts

    def within(layer):
        rows = []
        for shift in range(3):
            for pair in range(2):
                for r in (1, 0):
                    for y in range(2):
                        rows.append(
                            jnp.concatenate(
                                [unique[layer, r + 1 - to, 2 * pair + y, shift] for to in (1, 0)], axis=1
                            )
                        )
        return jnp.concatenate(rows, axis=0)

    def across(layer):
        rows = []
        none = jnp.zeros((64, 128), BF16)
        for shift in range(3):
            for pair in range(2):
                for y in range(2):
                    rows.append(jnp.concatenate([none, unique[layer, 0, 2 * pair + y, shift]], axis=1))
                for y in range(2):
                    rows.append(jnp.concatenate([unique[layer, 2, 2 * pair + y, shift], none], axis=1))
        return jnp.concatenate(rows, axis=0)

    def finish(total, layer, count, first_row, there):
        row = first_row + 2 * iota((count, 1, 256), 0) + ((iota((count, 1, 256), 2) >> 6) & 1)
        inside = (row >= 0) & (row < grid_rows) & there
        value = jnp.maximum(total + bias[layer], 0.0).reshape(count, 128, 256)
        return value * jnp.where(inside, 1.0, 0.0)

    def late_cells(j, b):
        tile = win[1, 1 + j + (b & 1)].astype(F32)
        at = (b >> 1) * 4 + (1 - (b & 1)) * 2
        return tile[at : at + 1], tile[at + 1 : at + 2]

    windows = ((0, True), (1, later))

    def begin(w, there, first, count):
        def cells(j, b):
            tile = win[2 * w, j].astype(F32)
            return tile[2 * b : 2 * b + 1], tile[2 * b + 1 : 2 * b + 2]

        put(ha, (w,), start(cells, first, count, base - 6, there), first, count)

    def first_layer(w, there, first, count):
        total = dot(jnp.concatenate(taps_of(ha, (w,), first, count), axis=1), within(0))
        put(hb, (w,), finish(total, 0, count, base - 5 + 2 * first, there), first, count)

    def middle_layer(w, there, first, count):
        total = dot(jnp.concatenate(taps_of(hb, (w,), first, count), axis=1), within(1))
        put(hc, (w,), finish(total, 1, count, base - 4 + 2 * first, there), first, count)

    def last_layer(w, there, first, count):
        total = dot(jnp.concatenate(taps_of(hc, (w,), first, count), axis=1), within(2))
        value = finish(total, 2, count, base - 3 + 2 * first, there)
        put(final, (w,), value[:, :, 128 * w : 128 * w + 128], first, count)
        if w == 0:
            ahead[first : first + count] = value[:, :, 128:256].astype(BF16)

    def pair_again(w, first, count):
        one, two = final[w, first : first + count].astype(F32), final[w, first + 1 : first + 1 + count].astype(F32)
        swapped = jnp.where(iota((count, 160, 128), 2) < 64, two, one)
        paired[w, first : first + count] = pltpu.roll(swapped, 64, 2).astype(BF16)

    pl.when(later)(to_earlier.wait_recv)
    for w, there in windows:
        begin(w, there, 3, 4)

    @pl.when(down)
    def _():
        pl.semaphore_wait(ready, 1)
        to_below.start()

    pl.when(down & later)(on_below.start)
    pl.when(up)(to_below.wait_recv)
    pl.when(up & later)(on_below.wait_recv)
    for w, there in windows:
        begin(w, there, 0, 3)
    for layer, count in ((first_layer, 6), (middle_layer, 5), (last_layer, 4)):
        for w, there in windows:
            layer(w, there, 0, count)
    put(hd, (0,), start(late_cells, 0, 5, base - 3, True), 0, 5)
    for w in range(2):
        pair_again(w, 0, 3)
    pl.when(down)(to_above.wait_recv)
    pl.when(down & later)(to_corner.wait_recv)
    for w, there in windows:
        begin(w, there, 7, 3)
    for layer, first in ((first_layer, 6), (middle_layer, 5), (last_layer, 4)):
        for w, there in windows:
            layer(w, there, first, 3)
    put(hd, (0,), start(late_cells, 5, 2, base - 3, True), 5, 2)
    for w in range(2):
        pair_again(w, 3, 3)

    def beside(ref, first, count):
        left = taps_of(ref, (0,), first, count)
        right = taps_of(ref, (1,), first, count)
        return [v for pair in zip(left, right) for v in pair]

    def second(own, others, layer, count, first_other):
        lhs = jnp.concatenate(taps_of(own, (0,), 0, count) + beside(others, first_other, count), axis=1)
        return dot(lhs, jnp.concatenate([within(layer), across(layer)], axis=0))

    put(hb, (0,), finish(second(hd, final, 0, 6, 0), 0, 6, base - 2, True), 0, 6)
    put(hc, (0,), finish(second(hb, paired, 1, 5, 0), 1, 5, base - 1, True), 0, 5)
    last = finish(second(hc, final, 2, 4, 1), 2, 4, base, True).astype(BF16).reshape(512, 256)

    w_terms = three_terms(quad(rw[...]))
    n = iota((32, 256), 0)
    weight = jnp.where(n >> 3 == 0, w_terms[0].astype(F32), jnp.where(n >> 3 == 1, w_terms[1].astype(F32), w_terms[2].astype(F32)))
    weight = jnp.where((n < 24) & ((n & 7) == iota((32, 256), 1) >> 6), weight, 0.0).astype(BF16)
    first = jnp.concatenate([final[0, 1:6, 16:144, :].reshape(640, 128), ahead[1:6].reshape(640, 128)], axis=1)
    a_sum = dot_nt(weight, first)
    b_sum = dot_nt(weight, last)
    a_sum = a_sum[0:8] + a_sum[8:16] + a_sum[16:24]
    b_sum = b_sum[0:8] + b_sum[8:16] + b_sum[16:24]
    y = iota((8, 128), 0)
    rounds = []
    for total, shift in ((a_sum, 1), (b_sum, 0)):
        for r in range(2):
            tile = jnp.zeros((8, 128), F32)
            for i in range(8):
                pair, inner = (i + shift) // 2, (i + shift) % 2
                b = (1 - r) * 2 + inner
                row = jnp.broadcast_to(total[b : b + 1, 128 * pair : 128 * pair + 128], (8, 128))
                tile = jnp.where(y == i, row, tile)
            rounds.append(tile)
    logits = jnp.concatenate(rounds, axis=0)
    back = one_hot(iota((128, 128), 1) == (iota((128, 128), 0) & 15) * 8 + (iota((128, 128), 0) >> 4))
    parts = dot(jnp.concatenate(three_terms(logits), axis=0), back)
    logits = (parts[0:32] + parts[32:64] + parts[64:96]).reshape(4, 8, 128)
    result[0] = logits
    out_ref[...] = logits

    pl.when(down)(to_below.wait_send)
    pl.when(up)(to_above.wait_send)
    pl.when(earlier)(to_earlier.wait_send)
    pl.when(later & down)(on_below.wait_send)
    pl.when(up & earlier)(to_corner.wait_send)


def kernel(
    spaces, times, lead,
    ev_hbm, so_hbm, emb_hbm, gain_hbm, cw_hbm, cb_hbm, rw_hbm,
    out_ref,
    ev, so, emb, gain, cw, cb, rw,
    win, unique, ha, hb, hc, hd, ahead, final, paired, result,
    load_sem, send_sem, recv_sem, hello, taker, ready,
):
    space, time, core = lax.axis_index("space"), lax.axis_index("tm"), lax.axis_index("chan")
    worker = core == lax.axis_size("chan") - 1
    grid_rows = 8 * spaces
    up, down = space > 0, space < spaces - 1
    later, earlier = time < times - 1, time > 0
    barrier = pltpu.get_barrier_semaphore()

    def remote(src, dst, sent, got, device):
        return pltpu.make_async_remote_copy(
            src_ref=src, dst_ref=dst, send_sem=send_sem.at[sent], recv_sem=recv_sem.at[got],
            device_id=device, device_id_type=MESH,
        )

    halfway, whole = lead
    far = whole > 1
    first = space == 0 if far else space < 0
    relay = space == halfway if far else space < 0
    keeper = space == whole if far else space < 0
    near = jnp.logical_not(first)
    give = remote(result.at[0], result.at[0], 5, 5, {"chan": core - 1})
    keep = remote(result.at[0], result.at[1], 6, 6, {"space": space + halfway, "chan": core - 1})
    pass_on = remote(result.at[1], result.at[1], 7, 6, {"space": space + whole - halfway})
    serve = remote(result.at[1], result.at[0], 7, 5, {"space": space - whole})

    def signal(there, semaphore, device):
        @pl.when(there)
        def _():
            pl.semaphore_signal(semaphore, inc=1, device_id=device, device_id_type=MESH)

    @pl.when(jnp.logical_not(worker))
    def _():
        signal(near, barrier, {"chan": core + 1})
        signal(relay, barrier, {"space": space + whole - halfway})
        signal(keeper, barrier, {"space": space - whole})

        @pl.when(first | relay | keeper)
        def _():
            pl.semaphore_wait(barrier, 1)

        signal(first, hello, {"space": space + whole})
        signal(relay, taker, {"space": space - halfway, "chan": core + 1})
        signal(keeper, taker, {"space": space + halfway - whole})

        @pl.when(relay)
        def _():
            keep.wait_recv()
            pl.semaphore_wait(taker, 1)
            pass_on.start()

        @pl.when(keeper)
        def _():
            pass_on.wait_recv()
            pl.semaphore_wait(hello, 1)
            serve.start()

        give.wait_recv()
        out_ref[...] = result[0]
        pl.when(relay)(pass_on.wait_send)
        pl.when(keeper)(serve.wait_send)

    @pl.when(worker)
    def _():
        loads = [
            pltpu.make_async_copy(src, dst, load_sem.at[i])
            for i, (src, dst) in enumerate(
                ((ev_hbm, ev), (so_hbm, so), (cw_hbm, cw), (emb_hbm, emb), (gain_hbm, gain), (cb_hbm, cb), (rw_hbm, rw))
            )
        ]
        for load in loads:
            load.start()

        signal(first, barrier, {"space": space + halfway, "chan": core - 1})
        signal(down, barrier, {"space": space + 1})
        signal(later, barrier, {"tm": time + 1})
        signal(earlier, barrier, {"tm": time - 1})
        signal(down & later, barrier, {"space": space + 1, "tm": time + 1})
        compute(
            spaces, space, time, near, up, down, later, earlier, barrier, ready, grid_rows, remote, loads,
            out_ref, ev, so, emb, gain, cw, cb, rw, win, unique, ha, hb, hc, hd, ahead, final, paired, result,
        )

        pl.when(near)(give.start)

        @pl.when(first)
        def _():
            pl.semaphore_wait(taker, 1)
            keep.start()

        pl.when(near)(give.wait_send)
        pl.when(first)(keep.wait_send)


def per_device(spaces, times, events, soft_info, embed, soft_gain, conv_weights, conv_bias, readout_weight):
    layers, channels, taps = conv_weights.shape
    gain = soft_gain.reshape(1, channels)
    readout = readout_weight.reshape(1, channels)
    whole = min(LEAD[1], spaces - 1)
    lead = min(LEAD[0], whole - 1), whole
    any_space = pl.BlockSpec(memory_space=pl.ANY)
    return pl.pallas_call(
        functools.partial(kernel, spaces, times, lead),
        out_shape=jax.ShapeDtypeStruct(events.shape, F32),
        in_specs=[any_space] * 7,
        out_specs=pl.BlockSpec(memory_space=pltpu.VMEM),
        scratch_shapes=[
            pltpu.VMEM(events.shape, jnp.int32),
            pltpu.VMEM(soft_info.shape, BF16),
            pltpu.VMEM(embed.shape, F32),
            pltpu.VMEM(gain.shape, F32),
            pltpu.VMEM(conv_weights.shape, BF16),
            pltpu.VMEM(conv_bias.shape, F32),
            pltpu.VMEM(readout.shape, F32),
            pltpu.VMEM((3, 10, 8, 128), BF16),
            pltpu.VMEM((layers, 3, 4, 3, channels, 128), BF16),
            pltpu.VMEM((2, 10, 160, 256), BF16),
            pltpu.VMEM((2, 9, 160, 256), BF16),
            pltpu.VMEM((2, 8, 160, 256), BF16),
            pltpu.VMEM((1, 7, 160, 256), BF16),
            pltpu.VMEM((7, 128, 128), BF16),
            pltpu.VMEM((2, 7, 160, 128), BF16),
            pltpu.VMEM((2, 6, 160, 128), BF16),
            pltpu.VMEM((2, *events.shape), F32),
            pltpu.SemaphoreType.DMA((7,)),
            pltpu.SemaphoreType.DMA((8,)),
            pltpu.SemaphoreType.DMA((7,)),
            pltpu.SemaphoreType.REGULAR,
            pltpu.SemaphoreType.REGULAR,
            pltpu.SemaphoreType.REGULAR,
        ],
        compiler_params=pltpu.CompilerParams(collective_id=0, has_side_effects=True, vmem_limit_bytes=48 * 1024 * 1024),
    )(*[pltpu.with_memory_space_constraint(v, pltpu.HBM) for v in (events, soft_info, embed, gain, conv_weights, conv_bias, readout)])


def solution(mesh):
    tiled = P(("parts", "tm"), "space", None)
    return jax.shard_map(
        functools.partial(per_device, mesh.shape["space"], mesh.shape["tm"]),
        mesh=mesh, in_specs=(tiled, tiled, P(), P(), P(), P(), P()), out_specs=tiled, check_vma=False,
    )
```
